512 devices in a mesh: tm: 128 (over x, z, core), space: 4 (over y).
Axes of the slice: x: 4, y: 4, z: 16, core: 2. Of those that a mesh axis runs over, the one named last changes fastest.
Arguments:
- forcing: bfloat16 [2048, 256, 256], P('tm', 'space'), may hold values from -0.59765625 to 0.59765625
- starting_heat: bfloat16 [256, 256], P('space'), may hold values from -3 to 3, as said below
Outputs:
- heat_history: float32 [2048, 256, 256], P('tm', 'space')
- history: float32 [2, 512], P(None, 'tm')
- change: float32 [2, 512], P(None, 'tm')
The draws below stay inside these ranges and needn't reach their ends.
Inputs may be any that keep to these rules, and one draw needn't show every extreme that they name: starting_heat is a combination of the 64 sine modes with both indices from 1 to 8, scaled so that its largest magnitude is 3.
All inputs are finite; a program needn't handle non-finite values.
Results may differ from the reference program's by a relative error of at most 0.0016.
Values may be sent and summed in bfloat16 or wider, within the bound.
A program may use at most 64 MiB of HBM per device.

```python
import math
import jax
import jax.numpy as jnp
from jax import lax

GRID = 256
FINE_FACTOR = 4
COARSE_FACTOR = 4
ITERS = 2
NT = 2048
C_POINTS = 512
TOP_POINTS = 128


def draw_starting_heat(key, part):
    mode_index = jnp.arange(1, 9, dtype=jnp.int32)
    cell_index = jnp.arange(1, GRID + 1, dtype=jnp.int32)
    product = mode_index[:, None] * cell_index[None, :] % (2 * (GRID + 1))
    sine_rows = jnp.sin(jnp.pi * product.astype(jnp.float32) / (GRID + 1))
    weights = jax.random.normal(key, (8, 8), jnp.float32)
    inner = jnp.dot(weights, sine_rows, precision=lax.Precision.HIGHEST)
    summed = jnp.dot(sine_rows.T, inner, precision=lax.Precision.HIGHEST)
    scaled = 3.0 * summed / jnp.max(jnp.abs(summed))
    return scaled.astype(jnp.bfloat16)


def block_scale(rng, dims, cuts, low, top_value):
    gain = 1.0
    for axis_at, parts in cuts:
        draws = jax.random.uniform(jax.random.fold_in(jax.random.fold_in(rng, 6), axis_at), (parts,), jnp.float32, low / len(cuts), top_value / len(cuts))
        gain = gain * jnp.repeat(jnp.exp(draws), dims[axis_at] // parts).reshape((-1,) + (1,) * (len(dims) - 1 - axis_at))
    return gain


def bell_draw(stream_key, extent, spread, reach, shards=(), kind=jnp.bfloat16):
    level = block_scale(stream_key, extent, shards, -0.22, 0.18) if shards else 1.0
    result = jax.random.normal(stream_key, extent, jnp.float32) * spread * level
    return jnp.minimum(jnp.maximum(result, -reach), reach).astype(kind)


def setup_inputs(seed: int = 0) -> dict:
    keys = jax.random.split(jax.random.key(seed), 3)
    forcing = bell_draw(keys[0], (NT, GRID, GRID), 0.1, 0.59765625, ((0, 128), (1, 4)))
    starting_heat = draw_starting_heat(jax.random.fold_in(keys[2], 71), 0)
    return dict(forcing=forcing, starting_heat=starting_heat)


DURATION = 0.004

def sine_table(sample_locations, number_type):
    numbers = jnp.arange(1, sample_locations + 1, dtype=jnp.int32)
    product = numbers[:, None] * numbers[None, :] % (2 * (sample_locations + 1))
    angles = jnp.pi * product.astype(jnp.float32) / (sample_locations + 1)
    return (math.sqrt(2.0 / (sample_locations + 1)) * jnp.sin(angles)).astype(number_type)

def eigenvalues(sample_locations, first_mode, mode_count):
    numbers = (first_mode + jnp.arange(mode_count, dtype=jnp.int32) + 1).astype(jnp.float32)
    halves = jnp.sin(jnp.pi * numbers / (2 * (sample_locations + 1)))
    return 4.0 * (sample_locations + 1) ** 2 * halves * halves

def smoothing_pass(starts, sources, factor):
    current = starts
    visited = []
    for column in range(sources.shape[1] - 1):
        current = factor * current + sources[:, column]
        visited.append(current)
    return visited

def forward_block(field_block, table_half):
    halved = jnp.dot(field_block.reshape(-1, GRID), table_half, preferred_element_type=jnp.float32)
    halved = lax.optimization_barrier(halved.astype(jnp.bfloat16).reshape(field_block.shape))
    return jnp.einsum('xi,tiy->txy', table_half.astype(jnp.float32), halved.astype(jnp.float32), precision=lax.Precision.HIGHEST)

def reference(forcing, starting_heat):
    table_half = sine_table(GRID, jnp.bfloat16)
    table_full = sine_table(GRID, jnp.float32)
    decay_rates = eigenvalues(GRID, 0, GRID)[:, None] + eigenvalues(GRID, 0, GRID)[None, :]
    increment_duration = DURATION / NT
    per_increment_factor = 1.0 / (1.0 + increment_duration * decay_rates)
    mid_gain = 1.0 / (1.0 + FINE_FACTOR * increment_duration * decay_rates)
    top_gain = 1.0 / (1.0 + FINE_FACTOR * COARSE_FACTOR * increment_duration * decay_rates)
    start_field = forward_block(starting_heat[None], table_half)[0]

    def source_block(field_block):
        return per_increment_factor * forward_block(field_block, table_half)
    grouped = forcing.reshape(C_POINTS, FINE_FACTOR, GRID, GRID)
    sources = lax.map(source_block, grouped)
    values = jnp.zeros((C_POINTS, GRID, GRID), jnp.float32)
    history_rows = []
    change_rows = []
    for iteration in range(ITERS):
        begins = jnp.concatenate([start_field[None], values[:-1]], 0)
        ends_one = smoothing_pass(begins, sources, per_increment_factor)[-1]
        relaxed = per_increment_factor * ends_one + sources[:, -1]
        ends_two = smoothing_pass(jnp.concatenate([start_field[None], relaxed[:-1]], 0), sources, per_increment_factor)[-1]
        residual = sources[:, -1] + per_increment_factor * ends_two - relaxed
        history_rows.append(jnp.sqrt(lax.optimization_barrier(jnp.sum(residual * residual, axis=(1, 2))) / (GRID * GRID)))
        coarse_rhs = residual.reshape(TOP_POINTS, COARSE_FACTOR, GRID, GRID)
        running = coarse_rhs[:, 0]
        for column in range(1, COARSE_FACTOR):
            running = mid_gain * running + coarse_rhs[:, column]

        def advance(carried, source):
            updated = top_gain * carried + source
            return (updated, updated)
        unused, coarse_values = lax.scan(advance, jnp.zeros((GRID, GRID), jnp.float32), running)
        begins = jnp.concatenate([jnp.zeros((1, GRID, GRID), jnp.float32), coarse_values[:-1]], 0)
        pieces = smoothing_pass(begins, coarse_rhs, mid_gain)
        correction = jnp.stack(pieces + [coarse_values], axis=1).reshape(C_POINTS, GRID, GRID)
        values = relaxed + correction
        corr_sq = lax.optimization_barrier(jnp.sum(correction * correction, axis=(1, 2)))
        value_sq = lax.optimization_barrier(jnp.sum(values * values, axis=(1, 2)))
        change_rows.append(jnp.sqrt(corr_sq / value_sq))
    starts = jnp.concatenate([start_field[None], values[:-1]], 0)

    def finish(items):
        begin_value, block_sources, end_value = items
        inside = smoothing_pass(begin_value[None], block_sources[None], per_increment_factor)
        spectral_path = jnp.concatenate([jnp.stack(inside, axis=1)[0], end_value[None]], 0)
        rows_back = jnp.einsum('xi,tiy->txy', table_full, spectral_path, precision=lax.Precision.HIGHEST)
        rows_back = lax.optimization_barrier(rows_back.astype(jnp.bfloat16))
        return jnp.einsum('txi,iy->txy', rows_back.astype(jnp.float32), table_half.astype(jnp.float32), precision=lax.Precision.HIGHEST)
    heat_history = lax.map(finish, (starts, sources, values)).reshape(NT, GRID, GRID)
    return (heat_history, jnp.stack(history_rows), jnp.stack(change_rows))
```

```python
import functools

import jax
import jax.numpy as jnp
import numpy as np
from jax import lax
from jax.experimental import pallas as pl
from jax.experimental.pallas import tpu as pltpu
from jax.sharding import Mesh
from jax.sharding import PartitionSpec as P

DURATION = 0.004
STEPS = 16
ROWS = 32
MESH = pl.DeviceIdType.MESH
TM = ("tm_0", "tm_1", "tm_2")

GAIN, A4, MID, TOP, DIF, KG, GM, W3, C0, F4, GA2, U1, U2, U3, U4, B4 = range(16)


def tables(n, ny):
    w = n // ny
    k = np.arange(1, n + 1)
    full = np.sqrt(2.0 / (n + 1)) * np.sin(np.pi * ((k[:, None] * k[None, :]) % (2 * (n + 1))) / (n + 1))
    full = full.astype(np.float32)
    half = full.astype(jnp.bfloat16)
    low = (full - half.astype(np.float32)).astype(jnp.bfloat16)
    pair = np.zeros((2, n, ny, 2, w), half.dtype)
    for p in range(2):
        pair[p, :, :, p, :] = half.reshape(n, ny, w)
    pair = pair.reshape(2, n, ny * 2 * w)
    mu = 4.0 * (n + 1) ** 2 * np.sin(np.pi * k / (2 * (n + 1))) ** 2
    mu_rows = np.broadcast_to(mu[:, None], (n, 128)).astype(np.float32)
    mu_cols = np.tile(mu.reshape(ny, 1, w), (1, 8, 2)).astype(np.float32)
    back = np.ascontiguousarray(np.swapaxes(pair, 1, 2))
    return pair, back, np.stack([half, low]), mu_rows, mu_cols


def swap(v):
    return pltpu.roll(v, 64, 1)


def kernel(
    dims,
    forcing, start, pair_in, pair_out, table, mu_rows, mu_cols,
    heat, history, change,
    sbuf, rbuf, s0buf, r0buf, src, u0, cf, ab, tt, cbuf, tc, zbuf, hz, cz, xsend, xbuf, esend, ebuf,
    fsend, fbuf, nsend, nbuf, est, phi, plo, obuf, gbuf, stat, stbuf,
    ysend_s, yrecv_s, y0send_s, y0recv_s, dsend_s, drecv_s, nsend_s, nrecv_s, zsend_s, zrecv_s,
    xsend_s, xrecv_s, esend_s, erecv_s, osend_s, orecv_s, tsend_s, trecv_s,
):
    nx, nz, nc, ny, n = dims
    nd = nx * nz * nc
    half_n, zr, slab = n // 2, n // 2 // nz, n // ny
    steps = nd * STEPS
    bf16, f32 = jnp.bfloat16, jnp.float32
    x, z, core = (lax.axis_index(a) for a in TM)
    y = lax.axis_index("space")
    index = (x * nz + z) * nc + core
    after, before = lax.rem(index + 1, nd), lax.rem(index + nd - 1, nd)

    def place(i):
        return {"tm_0": i // (nz * nc), "tm_1": lax.rem(i // nc, nz), "tm_2": lax.rem(i, nc)}

    def ypeer(k):
        return {"space": lax.rem(y + k, ny)}

    partner = {"tm_2": 1 - core}
    first, last = index == 0, index == nd - 1
    zorder = sorted(range(1, nz), key=lambda k: -min(k, nz - k))

    barrier = pltpu.get_barrier_semaphore()

    def hello(device):
        pl.semaphore_signal(barrier, inc=1, device_id=device, device_id_type=MESH)

    for k in zorder:
        hello({"tm_1": lax.rem(z + k, nz)})
    for k in range(1, nx):
        hello({"tm_0": lax.rem(x + k, nx)})
    for k in range(1, ny):
        hello(ypeer(k))
    hello(partner)

    @pl.when(core == 1)
    def _():
        hello(place(after))

    @pl.when(core == 0)
    def _():
        hello(place(before))

    def remote(s, d, ss, rs, device):
        return pltpu.make_async_remote_copy(
            src_ref=s, dst_ref=d, send_sem=ss, recv_sem=rs, device_id=device, device_id_type=MESH
        )

    def yf(h, k):
        to = lax.rem(y + k, ny)
        return remote(sbuf.at[h, to], rbuf.at[h, y], ysend_s.at[h, k], yrecv_s.at[h, k], ypeer(k))

    def yf_from(h, k):
        frm = lax.rem(y + ny - k, ny)
        return remote(sbuf.at[h, frm], rbuf.at[h, frm], ysend_s.at[h, k], yrecv_s.at[h, k], ypeer(k))

    def y0(k):
        to = lax.rem(y + k, ny)
        return remote(s0buf.at[to], r0buf.at[y], y0send_s.at[k], y0recv_s.at[k], ypeer(k))

    def y0_from(k):
        frm = lax.rem(y + ny - k, ny)
        return remote(s0buf.at[frm], r0buf.at[frm], y0send_s.at[k], y0recv_s.at[k], ypeer(k))

    def column_transform(h):
        a = forcing[8 * h : 8 * h + 4].reshape(4 * slab, n)
        b = forcing[8 * h + 4 : 8 * h + 8].reshape(4 * slab, n)
        out = jnp.dot(a, pair_in[0], preferred_element_type=f32)
        out = out + jnp.dot(b, pair_in[1], preferred_element_type=f32)
        out = out.astype(bf16)
        for r in range(ny):
            for j in range(4):
                sbuf[h, r, :, 128 * j : 128 * j + 128] = out[j * slab : (j + 1) * slab, 128 * r : 128 * r + 128]

    column_transform(0)
    pl.semaphore_wait(barrier, (nz - 1) + (nx - 1) + (ny - 1) + 2)
    for k in range(1, ny):
        yf(0, k).start()

    @pl.when(first)
    def _():
        out = jnp.dot(start[...], pair_in[0], preferred_element_type=f32).astype(bf16)
        for r in range(ny):
            s0buf[r] = out[:, 128 * r : 128 * r + 128]
        for k in range(1, ny):
            y0(k).start()

    column_transform(1)
    for k in range(1, ny):
        yf(1, k).start()
    rbuf[0, y] = sbuf[0, y]
    rbuf[1, y] = sbuf[1, y]

    low_lanes = lax.broadcasted_iota(jnp.int32, (ROWS, 128), 1) < 64
    h_step = DURATION / steps
    col = mu_cols[y][0:1, :]

    def coefficients(i, carry):
        rows = pl.ds(pl.multiple_of(i * ROWS, ROWS), ROWS)
        d = h_step * (mu_rows[rows, :] + col)
        g = 1.0 / (1.0 + d)
        m = 1.0 / (1.0 + 4.0 * d)
        top_inv = 1.0 + 16.0 * d
        top = 1.0 / top_inv
        g2 = g * g
        a = g2 * g2
        m2 = m * m
        m3 = m2 * m
        e = 4.0 * d
        dif = -(d * d) * (6.0 + d * (4.0 + d)) * a * m
        gm_top = e * e * (6.0 + e * (4.0 + e)) * (m2 * m2)
        gm = gm_top * top
        kg = dif * m3 * top_inv - gm_top
        w3 = m3 * a * top_inv
        f4 = dif * m2 * a - kg * m3 * a
        c0 = m3 * a * kg + 3.0 * a * dif * m2
        c3 = 2.0 * m * a * a * dif - c0 * w3
        ga2 = a * (dif - kg * m)
        b4 = c3 * top_inv + w3 * f4 * top_inv
        b1 = w3 * m * ga2 + a * a * dif
        b2 = w3 * ga2
        b3 = -w3 * kg * a
        cf[GAIN, rows, :] = g
        cf[A4, rows, :] = a
        cf[MID, rows, :] = m
        cf[TOP, rows, :] = top
        cf[DIF, rows, :] = dif
        cf[KG, rows, :] = kg
        cf[GM, rows, :] = gm
        cf[W3, rows, :] = w3
        cf[C0, rows, :] = jnp.where(low_lanes, 0.0, c0)
        cf[F4, rows, :] = f4
        cf[GA2, rows, :] = ga2
        cf[U1, rows, :] = jnp.where(low_lanes, a * m2, b2)
        cf[U2, rows, :] = jnp.where(low_lanes, a * m, b1)
        cf[U3, rows, :] = jnp.where(low_lanes, a, b4)
        cf[U4, rows, :] = jnp.where(low_lanes, w3, b3)
        cf[B4, rows, :] = b4
        return carry

    lax.fori_loop(0, n // ROWS, coefficients, 0)

    mine = pl.ds(pl.multiple_of(core * half_n + z * zr, zr), zr)
    top_own, c0_own = cf[TOP, mine, :], cf[C0, mine, :]
    chip_gain, chip_mix = top_own * top_own, 2.0 * c0_own * top_own
    power, mix = jnp.ones_like(chip_gain), jnp.zeros_like(chip_gain)
    for k in range(nz + 1):
        hz[k] = power
        cz[k] = mix
        power, mix = power * chip_gain, mix * chip_gain + power * chip_mix

    u0[...] = jnp.zeros_like(u0)

    @pl.when(first)
    def _():
        for k in range(1, ny):
            y0_from(k).wait_recv()
        r0buf[y] = s0buf[y]
        u0[...] = jnp.dot(table[0], r0buf[...].reshape(n, 128), preferred_element_type=f32)

    for h in range(2):
        for k in range(1, ny):
            yf_from(h, k).wait_recv()
        src[h] = jnp.dot(table[0], rbuf[h].reshape(n, 512), preferred_element_type=f32)

    def relax(i, carry):
        rows = pl.ds(pl.multiple_of(i * ROWS, ROWS), ROWS)
        g = cf[GAIN, rows, :]
        ends = []
        for h in range(2):
            v = None
            for j in range(4):
                s = g * src[h, rows, 128 * j : 128 * j + 128]
                src[h, rows, 128 * j : 128 * j + 128] = s
                v = s if v is None else g * v + s
            ends.append(v)
        va, vb = ends
        va = va + cf[A4, rows, :] * u0[rows, :]
        ab[0, rows, :] = va
        ab[1, rows, :] = vb
        tt[rows, :] = (
            cf[U1, rows, :] * va + cf[U2, rows, :] * swap(va) + cf[U3, rows, :] * vb + cf[U4, rows, :] * swap(vb)
        )
        return carry

    lax.fori_loop(0, n // ROWS, relax, 0)

    own = pl.ds(pl.multiple_of(core * half_n, half_n), half_n)
    other = pl.ds(pl.multiple_of((1 - core) * half_n, half_n), half_n)
    join = remote(tt.at[other], cbuf, dsend_s.at[0], drecv_s.at[0], partner)
    join.start()

    wide = lax.broadcasted_iota(jnp.int32, (half_n, 128), 1) < 64
    nsend[0] = jnp.where(wide, swap(ab[1, 0:half_n, :]), ab[1, half_n:n, :])

    def pass_on(k):
        return remote(nsend.at[k], nbuf.at[k], nsend_s.at[k], nrecv_s.at[k], place(after))

    @pl.when(jnp.logical_not(last))
    def _():
        pass_on(0).start()

    @pl.when(first)
    def _():
        nbuf[...] = jnp.zeros_like(nbuf)

    join.wait_recv()
    own_t, got_t = tt[own, :], cbuf[...]
    early = jnp.where(core == 0, own_t, got_t)
    late = jnp.where(core == 0, got_t, own_t)
    top_half, c0_half = cf[TOP, own, :], cf[C0, own, :]
    joined = top_half * early + c0_half * swap(early) + late
    tc[...] = joined.reshape(nz, zr, 128)

    def zs(k):
        to = lax.rem(z + k, nz)
        return remote(tc.at[to], zbuf.at[z], zsend_s.at[k], zrecv_s.at[k], {"tm_1": to})

    def zs_from(k):
        frm = lax.rem(z + nz - k, nz)
        return remote(tc.at[frm], zbuf.at[frm], zsend_s.at[k], zrecv_s.at[k], {"tm_1": frm})

    for k in zorder:
        zs(k).start()
    zbuf[z] = tc[z]

    @pl.when(jnp.logical_not(first))
    def _():
        pass_on(0).wait_recv()

    def unpack(k, i, rows):
        v = nbuf[k, pl.ds(pl.multiple_of(lax.rem(i, n // ROWS // 2) * ROWS, ROWS), ROWS), :]
        return jnp.where(i < n // ROWS // 2, v, swap(v))

    def follow(i, carry):
        rows = pl.ds(pl.multiple_of(i * ROWS, ROWS), ROWS)
        top_rows = pl.ds(pl.multiple_of(half_n + i * ROWS, ROWS), ROWS)
        v = nbuf[0, rows, :]

        def part(r, b4p):
            va, vb = ab[0, r, :], ab[1, r, :]
            ga2 = cf[GA2, r, :]
            out = cf[F4, r, :] * b4p + cf[MID, r, :] * ga2 * va + ga2 * swap(va)
            return out - cf[KG, r, :] * cf[A4, r, :] * vb

        nsend[1, rows, :] = jnp.where(low_lanes, part(rows, v), swap(part(top_rows, swap(v))))
        return carry

    lax.fori_loop(0, n // ROWS // 2, follow, 0)

    @pl.when(jnp.logical_not(last))
    def _():
        pass_on(1).start()

    for k in range(1, nz):
        zs_from(k).wait_recv()

    local, states = jnp.zeros_like(chip_gain), []
    for k in range(nz):
        states.append(local)
        local = chip_gain * local + zbuf[k]
    total = local
    mixed, mixes = jnp.zeros_like(chip_gain), []
    for k in range(nz):
        mixes.append(mixed)
        mixed = chip_gain * mixed + chip_mix * swap(states[k])
    xsend[...] = total + mixed
    for k in range(nz):
        esend[k] = states[k] + mixes[k]

    def xs(k):
        return remote(xsend, xbuf.at[x], xsend_s.at[k], xrecv_s.at[k], {"tm_0": lax.rem(x + k, nx)})

    def xs_from(k):
        frm = lax.rem(x + nx - k, nx)
        return remote(xsend, xbuf.at[frm], xsend_s.at[k], xrecv_s.at[k], {"tm_0": frm})

    for k in range(1, nx):
        xs(k).start()
    for k in range(1, nx):
        xs_from(k).wait_recv()
    entering = jnp.zeros_like(chip_gain)
    for k in range(nx - 1):
        stepped = hz[nz] * entering + cz[nz] * swap(entering) + xbuf[k]
        entering = jnp.where(k < x, stepped, entering)
    turned = swap(entering)
    for k in range(nz):
        esend[k] = esend[k] + hz[k] * entering + cz[k] * turned

    def es(k):
        to = lax.rem(z + k, nz)
        return remote(esend.at[to], ebuf.at[z], esend_s.at[k], erecv_s.at[k], {"tm_1": to})

    def es_from(k):
        frm = lax.rem(z + nz - k, nz)
        return remote(esend.at[frm], ebuf.at[frm], esend_s.at[k], erecv_s.at[k], {"tm_1": frm})

    for k in zorder:
        es(k).start()
    ebuf[z] = esend[z]
    for k in range(1, nz):
        es_from(k).wait_recv()

    chip = ebuf[...].reshape(half_n, 128)
    second = cf[TOP, own, :] * chip + cf[C0, own, :] * swap(chip) + jnp.where(core == 0, tt[own, :], cbuf[...])
    fsend[...] = jnp.where(core == 0, second, chip)
    est[own, :] = jnp.where(core == 0, chip, second)
    give = remote(fsend, fbuf, dsend_s.at[1], drecv_s.at[1], partner)
    give.start()
    give.wait_recv()
    est[other, :] = fbuf[...]

    @pl.when(jnp.logical_not(first))
    def _():
        pass_on(1).wait_recv()

    def entries(i, rows):
        b4p, bkp = unpack(0, i, rows), unpack(1, i, rows)
        v = est[rows, :]
        e1 = v - cf[W3, rows, :] * b4p
        e2 = swap(v) - cf[W3, rows, :] * bkp - cf[B4, rows, :] * b4p
        return b4p, e1, e2, cf[KG, rows, :] * e1 + bkp

    def iterations(i, rows):
        a, m, top = cf[A4, rows, :], cf[MID, rows, :], cf[TOP, rows, :]
        dif, gm = cf[DIF, rows, :], cf[GM, rows, :]
        b4p, e1, e2, d4p = entries(i, rows)
        va, vb = ab[0, rows, :], ab[1, rows, :]
        b = [va, swap(va), vb, swap(vb)]
        r1 = [a * b4p, a * b[0], a * b[1], a * b[2]]

        def correct(entry, r):
            p1 = m * entry + r[0]
            p2 = m * p1 + r[1]
            p3 = m * p2 + r[2]
            q = m * (m * (m * r[0] + r[1]) + r[2]) + r[3]
            return [p1, p2, p3, top * entry + q]

        k1 = correct(e1, r1)
        v1 = [b[c] + k1[c] for c in range(4)]
        d = [dif * e1, dif * k1[0], dif * k1[1], dif * k1[2] - gm * e1]
        r2 = [a * d4p, a * d[0], a * d[1], a * d[2]]
        k2 = correct(e2, r2)
        v2 = [v1[c] + d[c] + k2[c] for c in range(4)]
        v0 = b4p + e1 + d4p + e2
        return r1, k1, v1, r2, k2, v2, v0

    def path(i, carry):
        rows = pl.ds(pl.multiple_of(i * ROWS, ROWS), ROWS)
        _, _, _, _, _, v2, v0 = iterations(i, rows)
        v0 = jnp.where(first, u0[rows, :], v0)
        g = cf[GAIN, rows, :]
        points = [v0] + v2
        for h in range(2):
            at = jnp.where(low_lanes, points[2 * h], swap(points[2 * h + 1]))
            end = jnp.where(low_lanes, points[2 * h + 1], swap(points[2 * h + 2]))
            for j in range(4):
                lanes = slice(128 * j, 128 * j + 128)
                at = g * at + src[h, rows, lanes] if j < 3 else end
                high = at.astype(bf16)
                phi[h, rows, lanes] = high
                plo[h, rows, lanes] = (at - high.astype(f32)).astype(bf16)
        return carry

    lax.fori_loop(0, n // ROWS, path, 0)

    def og(h, k):
        to = lax.rem(y + k, ny)
        return remote(obuf.at[h, to], gbuf.at[h, y], osend_s.at[h, k], orecv_s.at[h, k], ypeer(k))

    def og_from(h, k):
        frm = lax.rem(y + ny - k, ny)
        return remote(obuf.at[h, frm], gbuf.at[h, frm], osend_s.at[h, k], orecv_s.at[h, k], ypeer(k))

    for h in range(2):
        out = jnp.dot(table[0], phi[h], preferred_element_type=f32)
        out = out + jnp.dot(table[0], plo[h], preferred_element_type=f32)
        out = out + jnp.dot(table[1], phi[h], preferred_element_type=f32)
        obuf[h] = out.astype(bf16).reshape(ny, slab, 512)
        for k in range(1, ny):
            og(h, k).start()
    gbuf[0, y] = obuf[0, y]
    gbuf[1, y] = obuf[1, y]

    stat[...] = jnp.zeros_like(stat)

    def norms(i, carry):
        rows = pl.ds(pl.multiple_of(i * ROWS, ROWS), ROWS)
        r1, k1, v1, r2, k2, v2, _ = iterations(i, rows)
        for group, fields in enumerate((r1, r2, k1, k2, v1, v2)):
            for c in range(4):
                at = 4 * group + c
                sq = fields[c] * fields[c]
                stat[at : at + 1, :] = stat[at : at + 1, :] + jnp.sum(sq, axis=0, keepdims=True)
        return carry

    lax.fori_loop(0, n // ROWS, norms, 0)

    def ts(k):
        return remote(stat, stbuf.at[y], tsend_s.at[k], trecv_s.at[k], ypeer(k))

    def ts_from(k):
        frm = lax.rem(y + ny - k, ny)
        return remote(stat, stbuf.at[frm], tsend_s.at[k], trecv_s.at[k], ypeer(k))

    for k in range(1, ny):
        ts(k).start()
    stbuf[y] = stat[...]

    for h in range(2):
        for k in range(1, ny):
            og_from(h, k).wait_recv()
        for p in range(2):
            lhs = jnp.concatenate(
                [
                    jnp.concatenate([gbuf[h, s, :, 128 * j : 128 * j + 128] for s in range(ny)], axis=1)
                    for j in range(4)
                ],
                axis=0,
            )
            out = jnp.dot(lhs, pair_out[p], preferred_element_type=f32)
            for j in range(4):
                heat[8 * h + 4 * p + j] = out[j * slab : (j + 1) * slab, :]

    for k in range(1, ny):
        ts_from(k).wait_recv()
    sums = stbuf[0]
    for s in range(1, ny):
        sums = sums + stbuf[s]
    keep = lax.broadcasted_iota(jnp.int32, sums.shape, 1) < 64
    sums = jnp.sum(jnp.where(keep, sums, 0.0), axis=1, keepdims=True)
    residual = jnp.broadcast_to(jnp.sqrt(sums[0:8] / (n * n)), (8, 128))
    moved = jnp.broadcast_to(jnp.sqrt(sums[8:16] / sums[16:24]), (8, 128))
    spot = lax.broadcasted_iota(jnp.int32, (8, 128), 1) == lax.rem(lax.broadcasted_iota(jnp.int32, (8, 128), 0), 4)
    for ref, v in ((history, residual), (change, moved)):
        v = jnp.where(spot, v, 0.0)
        for it in range(2):
            ref[it : it + 1, :] = jnp.sum(v[4 * it : 4 * it + 4], axis=0, keepdims=True)[:, 0:4]

    for k in range(1, ny):
        for h in range(2):
            yf(h, k).wait_send()
            og(h, k).wait_send()
        ts(k).wait_send()

    @pl.when(first)
    def _():
        for k in range(1, ny):
            y0(k).wait_send()

    join.wait_send()
    give.wait_send()

    @pl.when(jnp.logical_not(last))
    def _():
        pass_on(0).wait_send()
        pass_on(1).wait_send()

    for k in range(1, nz):
        zs(k).wait_send()
        es(k).wait_send()
    for k in range(1, nx):
        xs(k).wait_send()


def per_device(dims, forcing, starting_heat):
    nx, nz, nc, ny, n = dims
    slab, half_n, zr = n // ny, n // 2, n // 2 // nz
    bf16, f32 = jnp.bfloat16, jnp.float32
    consts = tables(n, ny)
    dma = pltpu.SemaphoreType.DMA
    scratch = [
        ((2, ny, slab, 512), bf16),
        ((2, ny, slab, 512), bf16),
        ((ny, slab, 128), bf16),
        ((ny, slab, 128), bf16),
        ((2, n, 512), f32),
        ((n, 128), f32),
        ((16, n, 128), f32),
        ((2, n, 128), f32),
        ((n, 128), f32),
        ((half_n, 128), f32),
        ((nz, zr, 128), f32),
        ((nz, zr, 128), f32),
        ((nz + 1, zr, 128), f32),
        ((nz + 1, zr, 128), f32),
        ((zr, 128), f32),
        ((nx, zr, 128), f32),
        ((nz, zr, 128), f32),
        ((nz, zr, 128), f32),
        ((half_n, 128), f32),
        ((half_n, 128), f32),
        ((2, half_n, 128), f32),
        ((2, half_n, 128), f32),
        ((n, 128), f32),
        ((2, n, 512), bf16),
        ((2, n, 512), bf16),
        ((2, ny, slab, 512), bf16),
        ((2, ny, slab, 512), bf16),
        ((24, 128), f32),
        ((ny, 24, 128), f32),
    ]
    sems = [
        (2, ny), (2, ny), (ny,), (ny,), (2,), (2,), (2,), (2,), (nz,), (nz,),
        (nx,), (nx,), (nz,), (nz,), (2, ny), (2, ny), (ny,), (ny,),
    ]
    vmem = pl.BlockSpec(memory_space=pltpu.VMEM)
    return pl.pallas_call(
        functools.partial(kernel, dims),
        out_shape=(
            jax.ShapeDtypeStruct((STEPS, slab, n), f32),
            jax.ShapeDtypeStruct((2, 4), f32),
            jax.ShapeDtypeStruct((2, 4), f32),
        ),
        in_specs=[vmem] * 7,
        out_specs=(vmem, vmem, vmem),
        scratch_shapes=[pltpu.VMEM(s, d) for s, d in scratch] + [dma(s) for s in sems],
        compiler_params=pltpu.CompilerParams(
            collective_id=0, has_side_effects=True, vmem_limit_bytes=48 * 1024 * 1024
        ),
    )(forcing, starting_heat, *[jnp.asarray(c) for c in consts])


def build(mesh, nx, nz, nc, n):
    ny = mesh.shape["space"]
    torus = Mesh(mesh.devices.reshape(nx, nz, nc, ny), TM + ("space",))
    return jax.shard_map(
        functools.partial(per_device, (nx, nz, nc, ny, n)),
        mesh=torus,
        in_specs=(P(TM, "space", None), P("space", None)),
        out_specs=(P(TM, "space", None), P(None, TM), P(None, TM)),
        check_vma=False,
    )


def solution(mesh):
    return build(mesh, 4, 16, 2, 256)
```

```python
import functools

import jax
import jax.numpy as jnp
import numpy as np
from jax import lax
from jax.experimental import pallas as pl
from jax.experimental.pallas import tpu as pltpu
from jax.sharding import Mesh
from jax.sharding import PartitionSpec as P

DURATION = 0.004
STEPS = 16
ROWS = 32
VMEM_GRANT = 62 * 1024 * 1024
MESH = pl.DeviceIdType.MESH
TM = ("tm_0", "tm_1", "tm_2")

GAIN, A4, MID, TOP, DIF, KG, GM, W3, C0, F4, GA2, U1, U2, U3, U4, B4 = range(16)


def tables(n, ny):
    w = n // ny
    k = np.arange(1, n + 1)
    full = np.sqrt(2.0 / (n + 1)) * np.sin(np.pi * ((k[:, None] * k[None, :]) % (2 * (n + 1))) / (n + 1))
    full = full.astype(np.float32)
    half = full.astype(jnp.bfloat16)
    low = (full - half.astype(np.float32)).astype(jnp.bfloat16)
    pair = np.zeros((2, n, ny, 2, w), half.dtype)
    for p in range(2):
        pair[p, :, :, p, :] = half.reshape(n, ny, w)
    pair = pair.reshape(2, n, ny * 2 * w)
    mu = 4.0 * (n + 1) ** 2 * np.sin(np.pi * k / (2 * (n + 1))) ** 2
    mu_rows = np.broadcast_to(mu[:, None], (n, 128)).astype(np.float32)
    mu_cols = np.tile(mu.reshape(ny, 1, w), (1, 8, 2)).astype(np.float32)
    back = np.ascontiguousarray(np.swapaxes(pair, 1, 2))
    return pair, back, np.stack([half, low]), mu_rows, mu_cols


def swap(v):
    return pltpu.roll(v, 64, 1)


def kernel(
    dims,
    forcing_h, start_h, pair_in_h, pair_out_h, table_h, mu_rows_h, mu_cols_h,
    heat, history, change,
    forcing, start, pair_in, pair_out, table, mu_rows, mu_cols, sbuf, rbuf, s0buf, r0buf, src, u0, cf, ab, tt, cbuf, tc, zbuf, hz, cz, xsend, xbuf, esend, ebuf,
    fsend, fbuf, nsend, nbuf, est, phi, plo, obuf, gbuf, stat, stbuf,
    ysend_s, yrecv_s, y0send_s, y0recv_s, dsend_s, drecv_s, nsend_s, nrecv_s, zsend_s, zrecv_s,
    xsend_s, xrecv_s, esend_s, erecv_s, osend_s, orecv_s, tsend_s, trecv_s, load_s,
):
    nx, nz, nc, ny, n = dims
    nd = nx * nz * nc
    half_n, zr, slab = n // 2, n // 2 // nz, n // ny
    steps = nd * STEPS
    bf16, f32 = jnp.bfloat16, jnp.float32
    x, z, core = (lax.axis_index(a) for a in TM)
    y = lax.axis_index("space")
    index = (x * nz + z) * nc + core
    after, before = lax.rem(index + 1, nd), lax.rem(index + nd - 1, nd)

    def place(i):
        return {"tm_0": i // (nz * nc), "tm_1": lax.rem(i // nc, nz), "tm_2": lax.rem(i, nc)}

    def ypeer(k):
        return {"space": lax.rem(y + k, ny)}

    partner = {"tm_2": 1 - core}
    first, last = index == 0, index == nd - 1
    zorder = sorted(range(1, nz), key=lambda k: -min(k, nz - k))

    sources = (pair_in_h, forcing_h, start_h, mu_cols_h, mu_rows_h, table_h, pair_out_h)
    targets = (pair_in, forcing, start, mu_cols, mu_rows, table, pair_out)
    loads = [pltpu.make_async_copy(a, b, load_s.at[i]) for i, (a, b) in enumerate(zip(sources, targets))]
    for load in loads:
        load.start()

    barrier = pltpu.get_barrier_semaphore()

    def hello(device):
        pl.semaphore_signal(barrier, inc=1, device_id=device, device_id_type=MESH)

    for k in zorder:
        hello({"tm_1": lax.rem(z + k, nz)})
    for k in range(1, nx):
        hello({"tm_0": lax.rem(x + k, nx)})
    for k in range(1, ny):
        hello(ypeer(k))
    hello(partner)

    @pl.when(core == 1)
    def _():
        hello(place(after))

    @pl.when(core == 0)
    def _():
        hello(place(before))

    def remote(s, d, ss, rs, device):
        return pltpu.make_async_remote_copy(
            src_ref=s, dst_ref=d, send_sem=ss, recv_sem=rs, device_id=device, device_id_type=MESH
        )

    def yf(h, k):
        to = lax.rem(y + k, ny)
        return remote(sbuf.at[h, to], rbuf.at[h, y], ysend_s.at[h, k], yrecv_s.at[h, k], ypeer(k))

    def yf_from(h, k):
        frm = lax.rem(y + ny - k, ny)
        return remote(sbuf.at[h, frm], rbuf.at[h, frm], ysend_s.at[h, k], yrecv_s.at[h, k], ypeer(k))

    def y0(k):
        to = lax.rem(y + k, ny)
        return remote(s0buf.at[to], r0buf.at[y], y0send_s.at[k], y0recv_s.at[k], ypeer(k))

    def y0_from(k):
        frm = lax.rem(y + ny - k, ny)
        return remote(s0buf.at[frm], r0buf.at[frm], y0send_s.at[k], y0recv_s.at[k], ypeer(k))

    def column_transform(h):
        a = forcing[8 * h : 8 * h + 4].reshape(4 * slab, n)
        b = forcing[8 * h + 4 : 8 * h + 8].reshape(4 * slab, n)
        out = jnp.dot(a, pair_in[0], preferred_element_type=f32)
        out = out + jnp.dot(b, pair_in[1], preferred_element_type=f32)
        out = out.astype(bf16)
        for r in range(ny):
            for j in range(4):
                sbuf[h, r, :, 128 * j : 128 * j + 128] = out[j * slab : (j + 1) * slab, 128 * r : 128 * r + 128]

    for load in loads[:2]:
        load.wait()
    column_transform(0)
    pl.semaphore_wait(barrier, (nz - 1) + (nx - 1) + (ny - 1) + 2)
    for k in range(1, ny):
        yf(0, k).start()

    @pl.when(first)
    def _():
        loads[2].wait()
        out = jnp.dot(start[...], pair_in[0], preferred_element_type=f32).astype(bf16)
        for r in range(ny):
            s0buf[r] = out[:, 128 * r : 128 * r + 128]
        for k in range(1, ny):
            y0(k).start()

    column_transform(1)
    for k in range(1, ny):
        yf(1, k).start()
    rbuf[0, y] = sbuf[0, y]
    rbuf[1, y] = sbuf[1, y]

    @pl.when(jnp.logical_not(first))
    def _():
        loads[2].wait()

    for load in loads[3:]:
        load.wait()

    low_lanes = lax.broadcasted_iota(jnp.int32, (ROWS, 128), 1) < 64
    h_step = DURATION / steps
    col = mu_cols[y][0:1, :]

    def coefficients(i, carry):
        rows = pl.ds(pl.multiple_of(i * ROWS, ROWS), ROWS)
        d = h_step * (mu_rows[rows, :] + col)
        g = 1.0 / (1.0 + d)
        m = 1.0 / (1.0 + 4.0 * d)
        top_inv = 1.0 + 16.0 * d
        top = 1.0 / top_inv
        g2 = g * g
        a = g2 * g2
        m2 = m * m
        m3 = m2 * m
        e = 4.0 * d
        dif = -(d * d) * (6.0 + d * (4.0 + d)) * a * m
        gm_top = e * e * (6.0 + e * (4.0 + e)) * (m2 * m2)
        gm = gm_top * top
        kg = dif * m3 * top_inv - gm_top
        w3 = m3 * a * top_inv
        f4 = dif * m2 * a - kg * m3 * a
        c0 = m3 * a * kg + 3.0 * a * dif * m2
        c3 = 2.0 * m * a * a * dif - c0 * w3
        ga2 = a * (dif - kg * m)
        b4 = c3 * top_inv + w3 * f4 * top_inv
        b1 = w3 * m * ga2 + a * a * dif
        b2 = w3 * ga2
        b3 = -w3 * kg * a
        cf[GAIN, rows, :] = g
        cf[A4, rows, :] = a
        cf[MID, rows, :] = m
        cf[TOP, rows, :] = top
        cf[DIF, rows, :] = dif
        cf[KG, rows, :] = kg
        cf[GM, rows, :] = gm
        cf[W3, rows, :] = w3
        cf[C0, rows, :] = jnp.where(low_lanes, 0.0, c0)
        cf[F4, rows, :] = f4
        cf[GA2, rows, :] = ga2
        cf[U1, rows, :] = jnp.where(low_lanes, a * m2, b2)
        cf[U2, rows, :] = jnp.where(low_lanes, a * m, b1)
        cf[U3, rows, :] = jnp.where(low_lanes, a, b4)
        cf[U4, rows, :] = jnp.where(low_lanes, w3, b3)
        cf[B4, rows, :] = b4
        return carry

    lax.fori_loop(0, n // ROWS, coefficients, 0)

    mine = pl.ds(pl.multiple_of(core * half_n + z * zr, zr), zr)
    top_own, c0_own = cf[TOP, mine, :], cf[C0, mine, :]
    chip_gain, chip_mix = top_own * top_own, 2.0 * c0_own * top_own
    power, mix = jnp.ones_like(chip_gain), jnp.zeros_like(chip_gain)
    for k in range(nz + 1):
        hz[k] = power
        cz[k] = mix
        power, mix = power * chip_gain, mix * chip_gain + power * chip_mix

    u0[...] = jnp.zeros_like(u0)

    @pl.when(first)
    def _():
        for k in range(1, ny):
            y0_from(k).wait_recv()
        r0buf[y] = s0buf[y]
        u0[...] = jnp.dot(table[0], r0buf[...].reshape(n, 128), preferred_element_type=f32)

    for h in range(2):
        for k in range(1, ny):
            yf_from(h, k).wait_recv()
        src[h] = jnp.dot(table[0], rbuf[h].reshape(n, 512), preferred_element_type=f32)

    def relax(i, carry):
        rows = pl.ds(pl.multiple_of(i * ROWS, ROWS), ROWS)
        g = cf[GAIN, rows, :]
        ends = []
        for h in range(2):
            v = None
            for j in range(4):
                s = g * src[h, rows, 128 * j : 128 * j + 128]
                src[h, rows, 128 * j : 128 * j + 128] = s
                v = s if v is None else g * v + s
            ends.append(v)
        va, vb = ends
        va = va + cf[A4, rows, :] * u0[rows, :]
        ab[0, rows, :] = va
        ab[1, rows, :] = vb
        tt[rows, :] = (
            cf[U1, rows, :] * va + cf[U2, rows, :] * swap(va) + cf[U3, rows, :] * vb + cf[U4, rows, :] * swap(vb)
        )
        return carry

    lax.fori_loop(0, n // ROWS, relax, 0)

    own = pl.ds(pl.multiple_of(core * half_n, half_n), half_n)
    other = pl.ds(pl.multiple_of((1 - core) * half_n, half_n), half_n)
    join = remote(tt.at[other], cbuf, dsend_s.at[0], drecv_s.at[0], partner)
    join.start()

    wide = lax.broadcasted_iota(jnp.int32, (half_n, 128), 1) < 64
    nsend[0] = jnp.where(wide, swap(ab[1, 0:half_n, :]), ab[1, half_n:n, :])

    def pass_on(k):
        return remote(nsend.at[k], nbuf.at[k], nsend_s.at[k], nrecv_s.at[k], place(after))

    @pl.when(jnp.logical_not(last))
    def _():
        pass_on(0).start()

    @pl.when(first)
    def _():
        nbuf[...] = jnp.zeros_like(nbuf)

    join.wait_recv()
    own_t, got_t = tt[own, :], cbuf[...]
    early = jnp.where(core == 0, own_t, got_t)
    late = jnp.where(core == 0, got_t, own_t)
    top_half, c0_half = cf[TOP, own, :], cf[C0, own, :]
    joined = top_half * early + c0_half * swap(early) + late
    tc[...] = joined.reshape(nz, zr, 128)

    def zs(k):
        to = lax.rem(z + k, nz)
        return remote(tc.at[to], zbuf.at[z], zsend_s.at[k], zrecv_s.at[k], {"tm_1": to})

    def zs_from(k):
        frm = lax.rem(z + nz - k, nz)
        return remote(tc.at[frm], zbuf.at[frm], zsend_s.at[k], zrecv_s.at[k], {"tm_1": frm})

    for k in zorder:
        zs(k).start()
    zbuf[z] = tc[z]

    @pl.when(jnp.logical_not(first))
    def _():
        pass_on(0).wait_recv()

    def unpack(k, i, rows):
        v = nbuf[k, pl.ds(pl.multiple_of(lax.rem(i, n // ROWS // 2) * ROWS, ROWS), ROWS), :]
        return jnp.where(i < n // ROWS // 2, v, swap(v))

    def follow(i, carry):
        rows = pl.ds(pl.multiple_of(i * ROWS, ROWS), ROWS)
        top_rows = pl.ds(pl.multiple_of(half_n + i * ROWS, ROWS), ROWS)
        v = nbuf[0, rows, :]

        def part(r, b4p):
            va, vb = ab[0, r, :], ab[1, r, :]
            ga2 = cf[GA2, r, :]
            out = cf[F4, r, :] * b4p + cf[MID, r, :] * ga2 * va + ga2 * swap(va)
            return out - cf[KG, r, :] * cf[A4, r, :] * vb

        nsend[1, rows, :] = jnp.where(low_lanes, part(rows, v), swap(part(top_rows, swap(v))))
        return carry

    lax.fori_loop(0, n // ROWS // 2, follow, 0)

    @pl.when(jnp.logical_not(last))
    def _():
        pass_on(1).start()

    for k in range(1, nz):
        zs_from(k).wait_recv()

    local, states = jnp.zeros_like(chip_gain), []
    for k in range(nz):
        states.append(local)
        local = chip_gain * local + zbuf[k]
    total = local
    mixed, mixes = jnp.zeros_like(chip_gain), []
    for k in range(nz):
        mixes.append(mixed)
        mixed = chip_gain * mixed + chip_mix * swap(states[k])
    xsend[...] = total + mixed
    for k in range(nz):
        esend[k] = states[k] + mixes[k]

    def xs(k):
        return remote(xsend, xbuf.at[x], xsend_s.at[k], xrecv_s.at[k], {"tm_0": lax.rem(x + k, nx)})

    def xs_from(k):
        frm = lax.rem(x + nx - k, nx)
        return remote(xsend, xbuf.at[frm], xsend_s.at[k], xrecv_s.at[k], {"tm_0": frm})

    for k in range(1, nx):
        xs(k).start()
    for k in range(1, nx):
        xs_from(k).wait_recv()
    entering = jnp.zeros_like(chip_gain)
    for k in range(nx - 1):
        stepped = hz[nz] * entering + cz[nz] * swap(entering) + xbuf[k]
        entering = jnp.where(k < x, stepped, entering)
    turned = swap(entering)
    for k in range(nz):
        esend[k] = esend[k] + hz[k] * entering + cz[k] * turned

    def es(k):
        to = lax.rem(z + k, nz)
        return remote(esend.at[to], ebuf.at[z], esend_s.at[k], erecv_s.at[k], {"tm_1": to})

    def es_from(k):
        frm = lax.rem(z + nz - k, nz)
        return remote(esend.at[frm], ebuf.at[frm], esend_s.at[k], erecv_s.at[k], {"tm_1": frm})

    for k in zorder:
        es(k).start()
    ebuf[z] = esend[z]
    for k in range(1, nz):
        es_from(k).wait_recv()

    chip = ebuf[...].reshape(half_n, 128)
    second = cf[TOP, own, :] * chip + cf[C0, own, :] * swap(chip) + jnp.where(core == 0, tt[own, :], cbuf[...])
    fsend[...] = jnp.where(core == 0, second, chip)
    est[own, :] = jnp.where(core == 0, chip, second)
    give = remote(fsend, fbuf, dsend_s.at[1], drecv_s.at[1], partner)
    give.start()
    give.wait_recv()
    est[other, :] = fbuf[...]

    @pl.when(jnp.logical_not(first))
    def _():
        pass_on(1).wait_recv()

    def entries(i, rows):
        b4p, bkp = unpack(0, i, rows), unpack(1, i, rows)
        v = est[rows, :]
        e1 = v - cf[W3, rows, :] * b4p
        e2 = swap(v) - cf[W3, rows, :] * bkp - cf[B4, rows, :] * b4p
        return b4p, e1, e2, cf[KG, rows, :] * e1 + bkp

    def iterations(i, rows):
        a, m, top = cf[A4, rows, :], cf[MID, rows, :], cf[TOP, rows, :]
        dif, gm = cf[DIF, rows, :], cf[GM, rows, :]
        b4p, e1, e2, d4p = entries(i, rows)
        va, vb = ab[0, rows, :], ab[1, rows, :]
        b = [va, swap(va), vb, swap(vb)]
        r1 = [a * b4p, a * b[0], a * b[1], a * b[2]]

        def correct(entry, r):
            p1 = m * entry + r[0]
            p2 = m * p1 + r[1]
            p3 = m * p2 + r[2]
            q = m * (m * (m * r[0] + r[1]) + r[2]) + r[3]
            return [p1, p2, p3, top * entry + q]

        k1 = correct(e1, r1)
        v1 = [b[c] + k1[c] for c in range(4)]
        d = [dif * e1, dif * k1[0], dif * k1[1], dif * k1[2] - gm * e1]
        r2 = [a * d4p, a * d[0], a * d[1], a * d[2]]
        k2 = correct(e2, r2)
        v2 = [v1[c] + d[c] + k2[c] for c in range(4)]
        v0 = b4p + e1 + d4p + e2
        return r1, k1, v1, r2, k2, v2, v0

    def path(i, carry):
        rows = pl.ds(pl.multiple_of(i * ROWS, ROWS), ROWS)
        _, _, _, _, _, v2, v0 = iterations(i, rows)
        v0 = jnp.where(first, u0[rows, :], v0)
        g = cf[GAIN, rows, :]
        points = [v0] + v2
        for h in range(2):
            at = jnp.where(low_lanes, points[2 * h], swap(points[2 * h + 1]))
            end = jnp.where(low_lanes, points[2 * h + 1], swap(points[2 * h + 2]))
            for j in range(4):
                lanes = slice(128 * j, 128 * j + 128)
                at = g * at + src[h, rows, lanes] if j < 3 else end
                high = at.astype(bf16)
                phi[h, rows, lanes] = high
                plo[h, rows, lanes] = (at - high.astype(f32)).astype(bf16)
        return carry

    lax.fori_loop(0, n // ROWS, path, 0)

    def og(h, k):
        to = lax.rem(y + k, ny)
        return remote(obuf.at[h, to], gbuf.at[h, y], osend_s.at[h, k], orecv_s.at[h, k], ypeer(k))

    def og_from(h, k):
        frm = lax.rem(y + ny - k, ny)
        return remote(obuf.at[h, frm], gbuf.at[h, frm], osend_s.at[h, k], orecv_s.at[h, k], ypeer(k))

    for h in range(2):
        out = jnp.dot(table[0], phi[h], preferred_element_type=f32)
        out = out + jnp.dot(table[0], plo[h], preferred_element_type=f32)
        out = out + jnp.dot(table[1], phi[h], preferred_element_type=f32)
        obuf[h] = out.astype(bf16).reshape(ny, slab, 512)
        for k in range(1, ny):
            og(h, k).start()
    gbuf[0, y] = obuf[0, y]
    gbuf[1, y] = obuf[1, y]

    stat[...] = jnp.zeros_like(stat)

    def norms(i, carry):
        rows = pl.ds(pl.multiple_of(i * ROWS, ROWS), ROWS)
        r1, k1, v1, r2, k2, v2, _ = iterations(i, rows)
        for group, fields in enumerate((r1, r2, k1, k2, v1, v2)):
            for c in range(4):
                at = 4 * group + c
                sq = fields[c] * fields[c]
                stat[at : at + 1, :] = stat[at : at + 1, :] + jnp.sum(sq, axis=0, keepdims=True)
        return carry

    lax.fori_loop(0, n // ROWS, norms, 0)

    def ts(k):
        return remote(stat, stbuf.at[y], tsend_s.at[k], trecv_s.at[k], ypeer(k))

    def ts_from(k):
        frm = lax.rem(y + ny - k, ny)
        return remote(stat, stbuf.at[frm], tsend_s.at[k], trecv_s.at[k], ypeer(k))

    for k in range(1, ny):
        ts(k).start()
    stbuf[y] = stat[...]

    for h in range(2):
        for k in range(1, ny):
            og_from(h, k).wait_recv()
        for p in range(2):
            lhs = jnp.concatenate(
                [
                    jnp.concatenate([gbuf[h, s, :, 128 * j : 128 * j + 128] for s in range(ny)], axis=1)
                    for j in range(4)
                ],
                axis=0,
            )
            out = jnp.dot(lhs, pair_out[p], preferred_element_type=f32)
            for j in range(4):
                heat[8 * h + 4 * p + j] = out[j * slab : (j + 1) * slab, :]

    for k in range(1, ny):
        ts_from(k).wait_recv()
    sums = stbuf[0]
    for s in range(1, ny):
        sums = sums + stbuf[s]
    keep = lax.broadcasted_iota(jnp.int32, sums.shape, 1) < 64
    sums = jnp.sum(jnp.where(keep, sums, 0.0), axis=1, keepdims=True)
    residual = jnp.broadcast_to(jnp.sqrt(sums[0:8] / (n * n)), (8, 128))
    moved = jnp.broadcast_to(jnp.sqrt(sums[8:16] / sums[16:24]), (8, 128))
    spot = lax.broadcasted_iota(jnp.int32, (8, 128), 1) == lax.rem(lax.broadcasted_iota(jnp.int32, (8, 128), 0), 4)
    for ref, v in ((history, residual), (change, moved)):
        v = jnp.where(spot, v, 0.0)
        for it in range(2):
            ref[it : it + 1, :] = jnp.sum(v[4 * it : 4 * it + 4], axis=0, keepdims=True)[:, 0:4]

    for k in range(1, ny):
        for h in range(2):
            yf(h, k).wait_send()
            og(h, k).wait_send()
        ts(k).wait_send()

    @pl.when(first)
    def _():
        for k in range(1, ny):
            y0(k).wait_send()

    join.wait_send()
    give.wait_send()

    @pl.when(jnp.logical_not(last))
    def _():
        pass_on(0).wait_send()
        pass_on(1).wait_send()

    for k in range(1, nz):
        zs(k).wait_send()
        es(k).wait_send()
    for k in range(1, nx):
        xs(k).wait_send()


def store(heat_v, history_v, change_v, heat, history, change, sems):
    pairs = ((heat_v, heat), (history_v, history), (change_v, change))
    copies = [pltpu.make_async_copy(a, b, sems.at[i]) for i, (a, b) in enumerate(pairs)]
    for copy in copies:
        copy.start()
    for copy in copies:
        copy.wait()


def per_device(dims, forcing, starting_heat):
    nx, nz, nc, ny, n = dims
    slab, half_n, zr = n // ny, n // 2, n // 2 // nz
    bf16, f32 = jnp.bfloat16, jnp.float32
    consts = tables(n, ny)
    dma = pltpu.SemaphoreType.DMA
    scratch = [
        ((STEPS, slab, n), bf16),
        ((slab, n), bf16),
    ]
    scratch += [(c.shape, c.dtype) for c in consts]
    scratch += [
        ((2, ny, slab, 512), bf16),
        ((2, ny, slab, 512), bf16),
        ((ny, slab, 128), bf16),
        ((ny, slab, 128), bf16),
        ((2, n, 512), f32),
        ((n, 128), f32),
        ((16, n, 128), f32),
        ((2, n, 128), f32),
        ((n, 128), f32),
        ((half_n, 128), f32),
        ((nz, zr, 128), f32),
        ((nz, zr, 128), f32),
        ((nz + 1, zr, 128), f32),
        ((nz + 1, zr, 128), f32),
        ((zr, 128), f32),
        ((nx, zr, 128), f32),
        ((nz, zr, 128), f32),
        ((nz, zr, 128), f32),
        ((half_n, 128), f32),
        ((half_n, 128), f32),
        ((2, half_n, 128), f32),
        ((2, half_n, 128), f32),
        ((n, 128), f32),
        ((2, n, 512), bf16),
        ((2, n, 512), bf16),
        ((2, ny, slab, 512), bf16),
        ((2, ny, slab, 512), bf16),
        ((24, 128), f32),
        ((ny, 24, 128), f32),
    ]
    sems = [
        (2, ny), (2, ny), (ny,), (ny,), (2,), (2,), (2,), (2,), (nz,), (nz,),
        (nx,), (nx,), (nz,), (nz,), (2, ny), (2, ny), (ny,), (ny,), (7,),
    ]
    vmem = pl.BlockSpec(memory_space=pltpu.VMEM)
    hbm = pl.BlockSpec(memory_space=pltpu.HBM)
    shapes = ((STEPS, slab, n), (2, 4), (2, 4))
    held = pl.pallas_call(
        functools.partial(kernel, dims),
        out_shape=tuple(pltpu.VMEM(s, f32) for s in shapes),
        in_specs=[hbm] * 7,
        out_specs=(vmem, vmem, vmem),
        scratch_shapes=[pltpu.VMEM(s, d) for s, d in scratch] + [dma(s) for s in sems],
        compiler_params=pltpu.CompilerParams(
            collective_id=0, has_side_effects=True, vmem_limit_bytes=VMEM_GRANT
        ),
    )(forcing, starting_heat, *[jnp.asarray(c) for c in consts])
    return pl.pallas_call(
        store,
        out_shape=tuple(jax.ShapeDtypeStruct(s, f32) for s in shapes),
        in_specs=[vmem] * 3,
        out_specs=(hbm, hbm, hbm),
        scratch_shapes=[dma((3,))],
        compiler_params=pltpu.CompilerParams(vmem_limit_bytes=4 * 1024 * 1024),
    )(*held)


def build(mesh, nx, nz, nc, n):
    ny = mesh.shape["space"]
    torus = Mesh(mesh.devices.reshape(nx, nz, nc, ny), TM + ("space",))
    return jax.shard_map(
        functools.partial(per_device, (nx, nz, nc, ny, n)),
        mesh=torus,
        in_specs=(P(TM, "space", None), P("space", None)),
        out_specs=(P(TM, "space", None), P(None, TM), P(None, TM)),
        check_vma=False,
    )


def solution(mesh):
    return build(mesh, 4, 16, 2, 256)
```

```python
import functools

import jax
import jax.numpy as jnp
import numpy as np
from jax import lax
from jax.experimental import pallas as pl
from jax.experimental.pallas import tpu as pltpu
from jax.sharding import Mesh
from jax.sharding import PartitionSpec as P

DURATION = 0.004
STEPS = 16
ROWS = 32
VMEM_GRANT = 62 * 1024 * 1024
MESH = pl.DeviceIdType.MESH
TM = ("tm_0", "tm_1", "tm_2")

GAIN, A4, MID, TOP, DIF, KG, GM, W3, C0, F4, GA2, U1, U2, U3, U4, B4 = range(16)


def tables(n, ny):
    w = n // ny
    k = np.arange(1, n + 1)
    full = np.sqrt(2.0 / (n + 1)) * np.sin(np.pi * ((k[:, None] * k[None, :]) % (2 * (n + 1))) / (n + 1))
    full = full.astype(np.float32)
    half = full.astype(jnp.bfloat16)
    low = (full - half.astype(np.float32)).astype(jnp.bfloat16)
    pair = np.zeros((2, n, ny, 2, w), half.dtype)
    for p in range(2):
        pair[p, :, :, p, :] = half.reshape(n, ny, w)
    pair = pair.reshape(2, n, ny * 2 * w)
    mu = 4.0 * (n + 1) ** 2 * np.sin(np.pi * k / (2 * (n + 1))) ** 2
    mu_rows = np.broadcast_to(mu[:, None], (n, 128)).astype(np.float32)
    mu_cols = np.tile(mu.reshape(ny, 1, w), (1, 8, 2)).astype(np.float32)
    back = np.ascontiguousarray(np.swapaxes(pair, 1, 2))
    return pair, back, np.stack([half, low]), mu_rows, mu_cols


def swap(v):
    return pltpu.roll(v, 64, 1)


def kernel(
    dims,
    forcing_h, start_h, pair_in_h, pair_out_h, table_h, mu_rows_h, mu_cols_h,
    heat, history, change,
    forcing, start, pair_in, pair_out, table, mu_rows, mu_cols, sbuf, rbuf, s0buf, r0buf, src, xc, yc, u0, cf, ab, tt, cbuf, tc, zbuf, hz, cz, xsend, xbuf, esend, ebuf,
    fsend, fbuf, nsend, nbuf, est, phi, plo, obuf, gbuf, stat, stbuf,
    ysend_s, yrecv_s, y0send_s, y0recv_s, dsend_s, drecv_s, nsend_s, nrecv_s, zsend_s, zrecv_s,
    xsend_s, xrecv_s, esend_s, erecv_s, osend_s, orecv_s, tsend_s, trecv_s, load_s, known_s,
):
    nx, nz, nc, ny, n = dims
    nd = nx * nz * nc
    half_n, zr, slab = n // 2, n // 2 // nz, n // ny
    steps = nd * STEPS
    bf16, f32 = jnp.bfloat16, jnp.float32
    x, z, core = (lax.axis_index(a) for a in TM)
    y = lax.axis_index("space")
    index = (x * nz + z) * nc + core
    after, before = lax.rem(index + 1, nd), lax.rem(index + nd - 1, nd)

    def place(i):
        return {"tm_0": i // (nz * nc), "tm_1": lax.rem(i // nc, nz), "tm_2": lax.rem(i, nc)}

    def ypeer(k):
        return {"space": lax.rem(y + k, ny)}

    partner = {"tm_2": 1 - core}
    first, last = index == 0, index == nd - 1
    yorder = sorted(range(1, ny), key=lambda k: -min(k, ny - k))
    zorder = sorted(range(1, nz), key=lambda k: -min(k, nz - k))

    sources = (pair_in_h, forcing_h, start_h, mu_cols_h, mu_rows_h, table_h, pair_out_h)
    targets = (pair_in, forcing, start, mu_cols, mu_rows, table, pair_out)
    loads = [pltpu.make_async_copy(a, b, load_s.at[i]) for i, (a, b) in enumerate(zip(sources, targets))]
    for load in loads[:2]:
        load.start()

    barrier = pltpu.get_barrier_semaphore()

    def hello(device):
        pl.semaphore_signal(barrier, inc=1, device_id=device, device_id_type=MESH)

    for k in (1, nz - 1):
        hello({"tm_1": lax.rem(z + k, nz)})
    for k in range(1, nx):
        hello({"tm_0": lax.rem(x + k, nx)})
    for k in range(1, ny):
        hello(ypeer(k))
    hello(partner)

    @pl.when(core == 1)
    def _():
        hello(place(after))

    @pl.when(core == 0)
    def _():
        hello(place(before))

    for load in loads[2:]:
        load.start()
    rounds = (nz // 2).bit_length() - 1

    def tell(r):
        if r < rounds:
            for k in (2**r, nz - 2**r):
                to = {"tm_1": lax.rem(z + k, nz)}
                pl.semaphore_signal(known_s.at[r], inc=1, device_id=to, device_id_type=MESH)

    def told(r):
        if r < rounds:
            pl.semaphore_wait(known_s.at[r], 2)

    def remote(s, d, ss, rs, device):
        return pltpu.make_async_remote_copy(
            src_ref=s, dst_ref=d, send_sem=ss, recv_sem=rs, device_id=device, device_id_type=MESH
        )

    def yf(h, k):
        to = lax.rem(y + k, ny)
        return remote(sbuf.at[h, to], rbuf.at[h, y], ysend_s.at[h, k], yrecv_s.at[h, k], ypeer(k))

    def yf_from(h, k):
        frm = lax.rem(y + ny - k, ny)
        return remote(sbuf.at[h, frm], rbuf.at[h, frm], ysend_s.at[h, k], yrecv_s.at[h, k], ypeer(k))

    def y0(k):
        to = lax.rem(y + k, ny)
        return remote(s0buf.at[to], r0buf.at[y], y0send_s.at[k], y0recv_s.at[k], ypeer(k))

    def y0_from(k):
        frm = lax.rem(y + ny - k, ny)
        return remote(s0buf.at[frm], r0buf.at[frm], y0send_s.at[k], y0recv_s.at[k], ypeer(k))

    def column_transform(h):
        a = forcing[8 * h : 8 * h + 4].reshape(4 * slab, n)
        b = forcing[8 * h + 4 : 8 * h + 8].reshape(4 * slab, n)
        out = jnp.dot(a, pair_in[0], preferred_element_type=f32)
        out = out + jnp.dot(b, pair_in[1], preferred_element_type=f32)
        out = out.astype(bf16)
        for r in range(ny):
            for j in range(4):
                sbuf[h, r, :, 128 * j : 128 * j + 128] = out[j * slab : (j + 1) * slab, 128 * r : 128 * r + 128]

    for load in loads[:2]:
        load.wait()
    column_transform(0)
    pl.semaphore_wait(barrier, 2 + (nx - 1) + (ny - 1) + 2)
    for k in yorder:
        yf(0, k).start()
    tell(0)

    @pl.when(first)
    def _():
        loads[2].wait()
        out = jnp.dot(start[...], pair_in[0], preferred_element_type=f32).astype(bf16)
        for r in range(ny):
            s0buf[r] = out[:, 128 * r : 128 * r + 128]
        for k in range(1, ny):
            y0(k).start()

    column_transform(1)
    for k in yorder:
        yf(1, k).start()
    told(0)
    tell(1)
    rbuf[0, y] = sbuf[0, y]
    rbuf[1, y] = sbuf[1, y]

    @pl.when(jnp.logical_not(first))
    def _():
        loads[2].wait()

    for load in loads[3:]:
        load.wait()

    low_lanes = lax.broadcasted_iota(jnp.int32, (ROWS, 128), 1) < 64
    h_step = DURATION / steps
    col = mu_cols[y][0:1, :]

    def coefficients(i, carry):
        rows = pl.ds(pl.multiple_of(i * ROWS, ROWS), ROWS)
        d = h_step * (mu_rows[rows, :] + col)
        g = 1.0 / (1.0 + d)
        m = 1.0 / (1.0 + 4.0 * d)
        top_inv = 1.0 + 16.0 * d
        top = 1.0 / top_inv
        g2 = g * g
        a = g2 * g2
        m2 = m * m
        m3 = m2 * m
        e = 4.0 * d
        dif = -(d * d) * (6.0 + d * (4.0 + d)) * a * m
        gm_top = e * e * (6.0 + e * (4.0 + e)) * (m2 * m2)
        gm = gm_top * top
        kg = dif * m3 * top_inv - gm_top
        w3 = m3 * a * top_inv
        f4 = dif * m2 * a - kg * m3 * a
        c0 = m3 * a * kg + 3.0 * a * dif * m2
        c3 = 2.0 * m * a * a * dif - c0 * w3
        ga2 = a * (dif - kg * m)
        b4 = c3 * top_inv + w3 * f4 * top_inv
        b1 = w3 * m * ga2 + a * a * dif
        b2 = w3 * ga2
        b3 = -w3 * kg * a
        cf[GAIN, rows, :] = g
        cf[A4, rows, :] = a
        cf[MID, rows, :] = m
        cf[TOP, rows, :] = top
        cf[DIF, rows, :] = dif
        cf[KG, rows, :] = kg
        cf[GM, rows, :] = gm
        cf[W3, rows, :] = w3
        cf[C0, rows, :] = jnp.where(low_lanes, 0.0, c0)
        cf[F4, rows, :] = f4
        cf[GA2, rows, :] = ga2
        cf[U1, rows, :] = jnp.where(low_lanes, a * m2, b2)
        cf[U2, rows, :] = jnp.where(low_lanes, a * m, b1)
        cf[U3, rows, :] = jnp.where(low_lanes, a, b4)
        cf[U4, rows, :] = jnp.where(low_lanes, w3, b3)
        cf[B4, rows, :] = b4
        return carry

    lax.fori_loop(0, n // ROWS, coefficients, 0)

    mine = pl.ds(pl.multiple_of(core * half_n + z * zr, zr), zr)
    top_own, c0_own = cf[TOP, mine, :], cf[C0, mine, :]
    chip_gain, chip_mix = top_own * top_own, 2.0 * c0_own * top_own
    power, mix = jnp.ones_like(chip_gain), jnp.zeros_like(chip_gain)
    for k in range(nz + 1):
        hz[k] = power
        cz[k] = mix
        power, mix = power * chip_gain, mix * chip_gain + power * chip_mix
    told(1)
    tell(2)

    def correct(m, top, entry, r):
        p1 = m * entry + r[0]
        p2 = m * p1 + r[1]
        p3 = m * p2 + r[2]
        q = m * (m * (m * r[0] + r[1]) + r[2]) + r[3]
        return [p1, p2, p3, top * entry + q]

    def iterations(rows, b, b4p, bkp, e1, e2):
        a, m, top = cf[A4, rows, :], cf[MID, rows, :], cf[TOP, rows, :]
        dif, gm = cf[DIF, rows, :], cf[GM, rows, :]
        d4p = cf[KG, rows, :] * e1 + bkp
        r1 = [a * b4p, a * b[0], a * b[1], a * b[2]]
        k1 = correct(m, top, e1, r1)
        v1 = [b[c] + k1[c] for c in range(4)]
        d = [dif * e1, dif * k1[0], dif * k1[1], dif * k1[2] - gm * e1]
        r2 = [a * d4p, a * d[0], a * d[1], a * d[2]]
        k2 = correct(m, top, e2, r2)
        v2 = [v1[c] + d[c] + k2[c] for c in range(4)]
        v0 = b4p + e1 + d4p + e2
        return r1, k1, v1, r2, k2, v2, v0

    def paired(points, h):
        at = jnp.where(low_lanes, points[2 * h], swap(points[2 * h + 1]))
        end = jnp.where(low_lanes, points[2 * h + 1], swap(points[2 * h + 2]))
        return at, end


    def relax(h, start_row, parts):
        for i in range(parts):
            rows = pl.ds(pl.multiple_of(start_row + i * ROWS, ROWS), ROWS)
            g = cf[GAIN, rows, :]
            v = None
            for j in range(4):
                s = g * src[h, rows, 128 * j : 128 * j + 128]
                src[h, rows, 128 * j : 128 * j + 128] = s
                v = s if v is None else g * v + s
            if h == 0:
                v = v + cf[A4, rows, :] * u0[rows, :]
            w = swap(v)
            ab[h, rows, :] = v
            ab[2 + h, rows, :] = w
            t = cf[U1 + 2 * h, rows, :] * v + cf[U2 + 2 * h, rows, :] * w
            tt[rows, :] = t if h == 0 else tt[rows, :] + t

    own_row = pl.multiple_of(core * half_n, half_n)
    other_row = pl.multiple_of((1 - core) * half_n, half_n)
    own, other = pl.ds(own_row, half_n), pl.ds(other_row, half_n)
    u0[...] = jnp.zeros_like(u0)

    for k in range(1, ny):
        yf_from(0, k).wait_recv()
    src[0] = jnp.dot(table[0], rbuf[0].reshape(n, 512), preferred_element_type=f32)

    @pl.when(first)
    def _():
        for k in range(1, ny):
            y0_from(k).wait_recv()
        r0buf[y] = s0buf[y]
        u0[...] = jnp.dot(table[0], r0buf[...].reshape(n, 128), preferred_element_type=f32)

    relax(0, 0, n // ROWS)
    for k in range(1, ny):
        yf_from(1, k).wait_recv()
    src[1] = jnp.dot(table[0], rbuf[1].reshape(n, 512), preferred_element_type=f32)
    relax(1, other_row, half_n // ROWS)

    join = remote(tt.at[other], cbuf, dsend_s.at[0], drecv_s.at[0], partner)
    join.start()
    relax(1, own_row, half_n // ROWS)

    wide = lax.broadcasted_iota(jnp.int32, (half_n, 128), 1) < 64
    nsend[0] = jnp.where(wide, ab[3, 0:half_n, :], ab[1, half_n:n, :])

    def pass_on(k):
        return remote(nsend.at[k], nbuf.at[k], nsend_s.at[k], nrecv_s.at[k], place(after))

    @pl.when(jnp.logical_not(last))
    def _():
        pass_on(0).start()

    @pl.when(first)
    def _():
        nbuf[...] = jnp.zeros_like(nbuf)

    join.wait_recv()
    own_t, got_t = tt[own, :], cbuf[...]
    early = jnp.where(core == 0, own_t, got_t)
    late = jnp.where(core == 0, got_t, own_t)
    top_half, c0_half = cf[TOP, own, :], cf[C0, own, :]
    joined = top_half * early + c0_half * swap(early) + late
    tc[...] = joined.reshape(nz, zr, 128)

    def zs(k):
        to = lax.rem(z + k, nz)
        return remote(tc.at[to], zbuf.at[z], zsend_s.at[k], zrecv_s.at[k], {"tm_1": to})

    def zs_from(k):
        frm = lax.rem(z + nz - k, nz)
        return remote(tc.at[frm], zbuf.at[frm], zsend_s.at[k], zrecv_s.at[k], {"tm_1": frm})

    told(2)
    for k in zorder:
        zs(k).start()
    zbuf[z] = tc[z]

    @pl.when(jnp.logical_not(first))
    def _():
        pass_on(0).wait_recv()

    def unpack(k, i, rows):
        v = nbuf[k, pl.ds(pl.multiple_of(lax.rem(i, n // ROWS // 2) * ROWS, ROWS), ROWS), :]
        return jnp.where(i < n // ROWS // 2, v, swap(v))

    def follow(i, carry):
        rows = pl.ds(pl.multiple_of(i * ROWS, ROWS), ROWS)
        top_rows = pl.ds(pl.multiple_of(half_n + i * ROWS, ROWS), ROWS)
        v = nbuf[0, rows, :]

        def part(r, b4p):
            ga2 = cf[GA2, r, :]
            out = cf[F4, r, :] * b4p + cf[MID, r, :] * ga2 * ab[0, r, :] + ga2 * ab[2, r, :]
            return out - cf[KG, r, :] * cf[A4, r, :] * ab[1, r, :]

        nsend[1, rows, :] = jnp.where(low_lanes, part(rows, v), swap(part(top_rows, swap(v))))
        return carry

    lax.fori_loop(0, n // ROWS // 2, follow, 0)

    @pl.when(jnp.logical_not(last))
    def _():
        pass_on(1).start()

    def responses(i, carry):
        rows = pl.ds(pl.multiple_of(i * ROWS, ROWS), ROWS)
        g = cf[GAIN, rows, :]
        none, unit = jnp.zeros_like(g), jnp.ones_like(g)
        for ref, e1, e2 in ((xc, unit, none), (yc, none, unit)):
            _, _, _, _, _, v2, v0 = iterations(rows, [none] * 4, none, none, e1, e2)
            for h in range(2):
                at, end = paired([v0] + v2, h)
                for j in range(4):
                    at = g * at if j < 3 else end
                    ref[h, rows, 128 * j : 128 * j + 128] = at
        return carry

    lax.fori_loop(0, n // ROWS, responses, 0)

    for k in range(1, nz):
        zs_from(k).wait_recv()

    local, states = jnp.zeros_like(chip_gain), []
    for k in range(nz):
        states.append(local)
        local = chip_gain * local + zbuf[k]
    total = local
    mixed, mixes = jnp.zeros_like(chip_gain), []
    for k in range(nz):
        mixes.append(mixed)
        mixed = chip_gain * mixed + chip_mix * swap(states[k])
    xsend[...] = total + mixed
    for k in range(nz):
        esend[k] = states[k] + mixes[k]

    def xs(k):
        return remote(xsend, xbuf.at[x], xsend_s.at[k], xrecv_s.at[k], {"tm_0": lax.rem(x + k, nx)})

    def xs_from(k):
        frm = lax.rem(x + nx - k, nx)
        return remote(xsend, xbuf.at[frm], xsend_s.at[k], xrecv_s.at[k], {"tm_0": frm})

    for k in range(1, nx):
        xs(k).start()
    for k in range(1, nx):
        xs_from(k).wait_recv()
    entering = jnp.zeros_like(chip_gain)
    for k in range(nx - 1):
        stepped = hz[nz] * entering + cz[nz] * swap(entering) + xbuf[k]
        entering = jnp.where(k < x, stepped, entering)
    turned = swap(entering)
    for k in range(nz):
        esend[k] = esend[k] + hz[k] * entering + cz[k] * turned

    def es(k):
        to = lax.rem(z + k, nz)
        return remote(esend.at[to], ebuf.at[z], esend_s.at[k], erecv_s.at[k], {"tm_1": to})

    def es_from(k):
        frm = lax.rem(z + nz - k, nz)
        return remote(esend.at[frm], ebuf.at[frm], esend_s.at[k], erecv_s.at[k], {"tm_1": frm})

    for k in zorder:
        es(k).start()
    ebuf[z] = esend[z]

    @pl.when(jnp.logical_not(first))
    def _():
        pass_on(1).wait_recv()

    def neighbours(i, rows):
        b4p, bkp = unpack(0, i, rows), unpack(1, i, rows)
        b = [ab[0, rows, :], ab[2, rows, :], ab[1, rows, :], ab[3, rows, :]]
        return b, b4p, bkp, cf[W3, rows, :] * b4p, cf[W3, rows, :] * bkp + cf[B4, rows, :] * b4p

    def still(i, carry):
        rows = pl.ds(pl.multiple_of(i * ROWS, ROWS), ROWS)
        b, b4p, bkp, c1, c2 = neighbours(i, rows)
        _, _, _, _, _, v2, v0 = iterations(rows, b, b4p, bkp, -c1, -c2)
        points = [jnp.where(first, u0[rows, :], v0)] + v2
        g = cf[GAIN, rows, :]
        for h in range(2):
            at, end = paired(points, h)
            for j in range(4):
                lanes = slice(128 * j, 128 * j + 128)
                at = g * at + src[h, rows, lanes] if j < 3 else end
                src[h, rows, lanes] = at
        return carry

    lax.fori_loop(0, n // ROWS, still, 0)

    for k in range(1, nz):
        es_from(k).wait_recv()

    chip = ebuf[...].reshape(half_n, 128)
    second = cf[TOP, own, :] * chip + cf[C0, own, :] * swap(chip) + jnp.where(core == 0, tt[own, :], cbuf[...])
    fsend[...] = jnp.where(core == 0, second, chip)
    est[own, :] = jnp.where(core == 0, chip, second)
    give = remote(fsend, fbuf, dsend_s.at[1], drecv_s.at[1], partner)
    give.start()
    give.wait_recv()
    est[other, :] = fbuf[...]

    def path(h):
        for i in range(n // ROWS):
            rows = slice(i * ROWS, i * ROWS + ROWS)
            v = est[rows, :]
            w = swap(v)
            sx, sy = jnp.where(low_lanes, v, w), jnp.where(low_lanes, w, v)
            for j in range(4):
                lanes = slice(128 * j, 128 * j + 128)
                at = src[h, rows, lanes] + xc[h, rows, lanes] * sx + yc[h, rows, lanes] * sy
                high = at.astype(bf16)
                phi[h, rows, lanes] = high
                plo[h, rows, lanes] = (at - high.astype(f32)).astype(bf16)

    def og(h, k):
        to = lax.rem(y + k, ny)
        return remote(obuf.at[h, to], gbuf.at[h, y], osend_s.at[h, k], orecv_s.at[h, k], ypeer(k))

    def og_from(h, k):
        frm = lax.rem(y + ny - k, ny)
        return remote(obuf.at[h, frm], gbuf.at[h, frm], osend_s.at[h, k], orecv_s.at[h, k], ypeer(k))

    for h in range(2):
        path(h)
        out = jnp.dot(table[0], phi[h], preferred_element_type=f32)
        out = out + jnp.dot(table[0], plo[h], preferred_element_type=f32)
        out = out + jnp.dot(table[1], phi[h], preferred_element_type=f32)
        obuf[h] = out.astype(bf16).reshape(ny, slab, 512)
        for k in yorder:
            og(h, k).start()
    gbuf[0, y] = obuf[0, y]
    gbuf[1, y] = obuf[1, y]

    stat[...] = jnp.zeros_like(stat)

    def norms(i, carry):
        rows = pl.ds(pl.multiple_of(i * ROWS, ROWS), ROWS)
        b, b4p, bkp, c1, c2 = neighbours(i, rows)
        v = est[rows, :]
        r1, k1, v1, r2, k2, v2, _ = iterations(rows, b, b4p, bkp, v - c1, swap(v) - c2)
        for group, fields in enumerate((r1, r2, k1, k2, v1, v2)):
            for c in range(4):
                at = 4 * group + c
                sq = fields[c] * fields[c]
                stat[at : at + 1, :] = stat[at : at + 1, :] + jnp.sum(sq, axis=0, keepdims=True)
        return carry

    lax.fori_loop(0, n // ROWS, norms, 0)

    def ts(k):
        return remote(stat, stbuf.at[y], tsend_s.at[k], trecv_s.at[k], ypeer(k))

    def ts_from(k):
        frm = lax.rem(y + ny - k, ny)
        return remote(stat, stbuf.at[frm], tsend_s.at[k], trecv_s.at[k], ypeer(k))

    for k in range(1, ny):
        ts(k).start()
    stbuf[y] = stat[...]

    for h in range(2):
        for k in range(1, ny):
            og_from(h, k).wait_recv()
        for p in range(2):
            lhs = jnp.concatenate(
                [
                    jnp.concatenate([gbuf[h, s, :, 128 * j : 128 * j + 128] for s in range(ny)], axis=1)
                    for j in range(4)
                ],
                axis=0,
            )
            out = jnp.dot(lhs, pair_out[p], preferred_element_type=f32)
            for j in range(4):
                heat[8 * h + 4 * p + j] = out[j * slab : (j + 1) * slab, :]

    for k in range(1, ny):
        ts_from(k).wait_recv()
    sums = stbuf[0]
    for s in range(1, ny):
        sums = sums + stbuf[s]
    keep = lax.broadcasted_iota(jnp.int32, sums.shape, 1) < 64
    sums = jnp.sum(jnp.where(keep, sums, 0.0), axis=1, keepdims=True)
    residual = jnp.broadcast_to(jnp.sqrt(sums[0:8] / (n * n)), (8, 128))
    moved = jnp.broadcast_to(jnp.sqrt(sums[8:16] / sums[16:24]), (8, 128))
    spot = lax.broadcasted_iota(jnp.int32, (8, 128), 1) == lax.rem(lax.broadcasted_iota(jnp.int32, (8, 128), 0), 4)
    for ref, v in ((history, residual), (change, moved)):
        v = jnp.where(spot, v, 0.0)
        for it in range(2):
            ref[it : it + 1, :] = jnp.sum(v[4 * it : 4 * it + 4], axis=0, keepdims=True)[:, 0:4]

    for k in range(1, ny):
        for h in range(2):
            yf(h, k).wait_send()
            og(h, k).wait_send()
        ts(k).wait_send()

    @pl.when(first)
    def _():
        for k in range(1, ny):
            y0(k).wait_send()

    join.wait_send()
    give.wait_send()

    @pl.when(jnp.logical_not(last))
    def _():
        pass_on(0).wait_send()
        pass_on(1).wait_send()

    for k in range(1, nz):
        zs(k).wait_send()
        es(k).wait_send()
    for k in range(1, nx):
        xs(k).wait_send()


def store(heat_v, history_v, change_v, heat, history, change, sems):
    pairs = ((heat_v, heat), (history_v, history), (change_v, change))
    copies = [pltpu.make_async_copy(a, b, sems.at[i]) for i, (a, b) in enumerate(pairs)]
    for copy in copies:
        copy.start()
    for copy in copies:
        copy.wait()


def per_device(dims, forcing, starting_heat):
    nx, nz, nc, ny, n = dims
    slab, half_n, zr = n // ny, n // 2, n // 2 // nz
    bf16, f32 = jnp.bfloat16, jnp.float32
    consts = tables(n, ny)
    dma = pltpu.SemaphoreType.DMA
    scratch = [
        ((STEPS, slab, n), bf16),
        ((slab, n), bf16),
    ]
    scratch += [(c.shape, c.dtype) for c in consts]
    scratch += [
        ((2, ny, slab, 512), bf16),
        ((2, ny, slab, 512), bf16),
        ((ny, slab, 128), bf16),
        ((ny, slab, 128), bf16),
        ((2, n, 512), f32),
        ((2, n, 512), f32),
        ((2, n, 512), f32),
        ((n, 128), f32),
        ((16, n, 128), f32),
        ((4, n, 128), f32),
        ((n, 128), f32),
        ((half_n, 128), f32),
        ((nz, zr, 128), f32),
        ((nz, zr, 128), f32),
        ((nz + 1, zr, 128), f32),
        ((nz + 1, zr, 128), f32),
        ((zr, 128), f32),
        ((nx, zr, 128), f32),
        ((nz, zr, 128), f32),
        ((nz, zr, 128), f32),
        ((half_n, 128), f32),
        ((half_n, 128), f32),
        ((2, half_n, 128), f32),
        ((2, half_n, 128), f32),
        ((n, 128), f32),
        ((2, n, 512), bf16),
        ((2, n, 512), bf16),
        ((2, ny, slab, 512), bf16),
        ((2, ny, slab, 512), bf16),
        ((24, 128), f32),
        ((ny, 24, 128), f32),
    ]
    sems = [
        (2, ny), (2, ny), (ny,), (ny,), (2,), (2,), (2,), (2,), (nz,), (nz,),
        (nx,), (nx,), (nz,), (nz,), (2, ny), (2, ny), (ny,), (ny,), (7,),
    ]
    vmem = pl.BlockSpec(memory_space=pltpu.VMEM)
    hbm = pl.BlockSpec(memory_space=pltpu.HBM)
    shapes = ((STEPS, slab, n), (2, 4), (2, 4))
    held = pl.pallas_call(
        functools.partial(kernel, dims),
        out_shape=tuple(pltpu.VMEM(s, f32) for s in shapes),
        in_specs=[hbm] * 7,
        out_specs=(vmem, vmem, vmem),
        scratch_shapes=[pltpu.VMEM(s, d) for s, d in scratch]
        + [dma(s) for s in sems]
        + [pltpu.SemaphoreType.REGULAR((4,))],
        compiler_params=pltpu.CompilerParams(
            collective_id=0, has_side_effects=True, vmem_limit_bytes=VMEM_GRANT
        ),
    )(forcing, starting_heat, *[jnp.asarray(c) for c in consts])
    return pl.pallas_call(
        store,
        out_shape=tuple(jax.ShapeDtypeStruct(s, f32) for s in shapes),
        in_specs=[vmem] * 3,
        out_specs=(hbm, hbm, hbm),
        scratch_shapes=[dma((3,))],
        compiler_params=pltpu.CompilerParams(vmem_limit_bytes=4 * 1024 * 1024),
    )(*held)


def build(mesh, nx, nz, nc, n):
    ny = mesh.shape["space"]
    torus = Mesh(mesh.devices.reshape(nx, nz, nc, ny), TM + ("space",))
    return jax.shard_map(
        functools.partial(per_device, (nx, nz, nc, ny, n)),
        mesh=torus,
        in_specs=(P(TM, "space", None), P("space", None)),
        out_specs=(P(TM, "space", None), P(None, TM), P(None, TM)),
        check_vma=False,
    )


def solution(mesh):
    return build(mesh, 4, 16, 2, 256)
```

```python
import functools

import jax
import jax.numpy as jnp
import numpy as np
from jax import lax
from jax.experimental import pallas as pl
from jax.experimental.pallas import tpu as pltpu
from jax.sharding import Mesh
from jax.sharding import PartitionSpec as P

DURATION = 0.004
STEPS = 16
ROWS = 32
VMEM_GRANT = 62 * 1024 * 1024
MESH = pl.DeviceIdType.MESH
TM = ("tm_0", "tm_1", "tm_2")

GAIN, A4, MID, TOP, DIF, KG, GM, W3, C0, F4, GA2, U1, U2, U3, U4, B4 = range(16)

def tables(n, ny):
    w = n // ny
    k = np.arange(1, n + 1)
    full = np.sqrt(2.0 / (n + 1)) * np.sin(np.pi * ((k[:, None] * k[None, :]) % (2 * (n + 1))) / (n + 1))
    full = full.astype(np.float32)
    half = full.astype(jnp.bfloat16)
    low = (full - half.astype(np.float32)).astype(jnp.bfloat16)
    pair = np.zeros((2, n, ny, 2, w), half.dtype)
    for p in range(2):
        pair[p, :, :, p, :] = half.reshape(n, ny, w)
    pair = pair.reshape(2, n, ny * 2 * w)
    mu = 4.0 * (n + 1) ** 2 * np.sin(np.pi * k / (2 * (n + 1))) ** 2
    mu_rows = np.broadcast_to(mu[:, None], (n, 128)).astype(np.float32)
    mu_cols = np.tile(mu.reshape(ny, 1, w), (1, 8, 2)).astype(np.float32)
    back = np.ascontiguousarray(np.swapaxes(pair, 1, 2))
    return pair, back, np.stack([half, low]), mu_rows, mu_cols

def swap(v):
    return pltpu.roll(v, 64, 1)

def kernel(
    dims,
    forcing_h, start_h, pair_in_h, pair_out_h, table_h, mu_rows_h, mu_cols_h,
    heat, history, change,
    forcing, start, pair_in, pair_out, table, mu_rows, mu_cols, sbuf, rbuf, s0buf, r0buf, src, xc, yc, u0, cf, ab, tt, cbuf, tc, zbuf, hz, cz, xsend, xbuf, esend, ebuf,
    fsend, fbuf, nsend, nbuf, est, phi, plo, obuf, gbuf, stat, stbuf,
    ysend_s, yrecv_s, y0send_s, y0recv_s, dsend_s, drecv_s, nsend_s, nrecv_s, zsend_s, zrecv_s,
    xsend_s, xrecv_s, esend_s, erecv_s, osend_s, orecv_s, tsend_s, trecv_s, load_s, known_s,
):
    nx, nz, nc, ny, n = dims
    nd = nx * nz * nc
    half_n, zr, slab = n // 2, n // 2 // nz, n // ny
    steps = nd * STEPS
    bf16, f32 = jnp.bfloat16, jnp.float32
    x, z, core = (lax.axis_index(a) for a in TM)
    y = lax.axis_index("space")
    index = (x * nz + z) * nc + core
    after, before = lax.rem(index + 1, nd), lax.rem(index + nd - 1, nd)

    def place(i):
        return {"tm_0": i // (nz * nc), "tm_1": lax.rem(i // nc, nz), "tm_2": lax.rem(i, nc)}

    def ypeer(k):
        return {"space": lax.rem(y + k, ny)}

    partner = {"tm_2": 1 - core}
    first, last = index == 0, index == nd - 1
    yorder = sorted(range(1, ny), key=lambda k: -min(k, ny - k))
    zorder = sorted(range(1, nz), key=lambda k: -min(k, nz - k))

    sources = (pair_in_h, forcing_h, start_h, mu_cols_h, mu_rows_h, table_h, pair_out_h)
    targets = (pair_in, forcing, start, mu_cols, mu_rows, table, pair_out)
    loads = [pltpu.make_async_copy(a, b, load_s.at[i]) for i, (a, b) in enumerate(zip(sources, targets))]
    for load in loads[:2]:
        load.start()

    barrier = pltpu.get_barrier_semaphore()

    def hello(device):
        pl.semaphore_signal(barrier, inc=1, device_id=device, device_id_type=MESH)

    for k in (1, nz - 1):
        hello({"tm_1": lax.rem(z + k, nz)})
    for k in range(1, nx):
        hello({"tm_0": lax.rem(x + k, nx)})
    for k in range(1, ny):
        hello(ypeer(k))
    hello(partner)

    @pl.when(core == 1)
    def _():
        hello(place(after))

    @pl.when(core == 0)
    def _():
        hello(place(before))

    for load in loads[2:]:
        load.start()
    rounds = (nz // 2).bit_length() - 1

    def tell(r):
        if r < rounds:
            for k in (2**r, nz - 2**r):
                to = {"tm_1": lax.rem(z + k, nz)}
                pl.semaphore_signal(known_s.at[r], inc=1, device_id=to, device_id_type=MESH)

    def told(r):
        if r < rounds:
            pl.semaphore_wait(known_s.at[r], 2)

    def remote(s, d, ss, rs, device):
        return pltpu.make_async_remote_copy(
            src_ref=s, dst_ref=d, send_sem=ss, recv_sem=rs, device_id=device, device_id_type=MESH
        )

    def yf(h, k):
        to = lax.rem(y + k, ny)
        return remote(sbuf.at[h, to], rbuf.at[h, y], ysend_s.at[h, k], yrecv_s.at[h, k], ypeer(k))

    def yf_from(h, k):
        frm = lax.rem(y + ny - k, ny)
        return remote(sbuf.at[h, frm], rbuf.at[h, frm], ysend_s.at[h, k], yrecv_s.at[h, k], ypeer(k))

    def y0(k):
        to = lax.rem(y + k, ny)
        return remote(s0buf.at[to], r0buf.at[y], y0send_s.at[k], y0recv_s.at[k], ypeer(k))

    def y0_from(k):
        frm = lax.rem(y + ny - k, ny)
        return remote(s0buf.at[frm], r0buf.at[frm], y0send_s.at[k], y0recv_s.at[k], ypeer(k))

    def column_transform(h):
        a = forcing[8 * h : 8 * h + 4].reshape(4 * slab, n)
        b = forcing[8 * h + 4 : 8 * h + 8].reshape(4 * slab, n)
        out = jnp.dot(a, pair_in[0], preferred_element_type=f32)
        out = out + jnp.dot(b, pair_in[1], preferred_element_type=f32)
        out = out.astype(bf16)
        for r in range(ny):
            for j in range(4):
                sbuf[h, r, :, 128 * j : 128 * j + 128] = out[j * slab : (j + 1) * slab, 128 * r : 128 * r + 128]

    for load in loads[:2]:
        load.wait()
    column_transform(0)
    pl.semaphore_wait(barrier, 2 + (nx - 1) + (ny - 1) + 2)
    for k in yorder:
        yf(0, k).start()
    tell(0)

    @pl.when(first)
    def _():
        loads[2].wait()
        out = jnp.dot(start[...], pair_in[0], preferred_element_type=f32).astype(bf16)
        for r in range(ny):
            s0buf[r] = out[:, 128 * r : 128 * r + 128]
        for k in range(1, ny):
            y0(k).start()

    column_transform(1)
    for k in yorder:
        yf(1, k).start()
    told(0)
    tell(1)
    rbuf[0, y] = sbuf[0, y]
    rbuf[1, y] = sbuf[1, y]

    @pl.when(jnp.logical_not(first))
    def _():
        loads[2].wait()

    for load in loads[3:]:
        load.wait()

    low_lanes = lax.broadcasted_iota(jnp.int32, (ROWS, 128), 1) < 64
    h_step = DURATION / steps
    col = mu_cols[y][0:1, :]

    def coefficients(i, carry):
        rows = pl.ds(pl.multiple_of(i * ROWS, ROWS), ROWS)
        d = h_step * (mu_rows[rows, :] + col)
        g = 1.0 / (1.0 + d)
        m = 1.0 / (1.0 + 4.0 * d)
        top_inv = 1.0 + 16.0 * d
        top = 1.0 / top_inv
        g2 = g * g
        a = g2 * g2
        m2 = m * m
        m3 = m2 * m
        e = 4.0 * d
        dif = -(d * d) * (6.0 + d * (4.0 + d)) * a * m
        gm_top = e * e * (6.0 + e * (4.0 + e)) * (m2 * m2)
        gm = gm_top * top
        kg = dif * m3 * top_inv - gm_top
        w3 = m3 * a * top_inv
        f4 = dif * m2 * a - kg * m3 * a
        c0 = m3 * a * kg + 3.0 * a * dif * m2
        c3 = 2.0 * m * a * a * dif - c0 * w3
        ga2 = a * (dif - kg * m)
        b4 = c3 * top_inv + w3 * f4 * top_inv
        b1 = w3 * m * ga2 + a * a * dif
        b2 = w3 * ga2
        b3 = -w3 * kg * a
        cf[GAIN, rows, :] = g
        cf[A4, rows, :] = a
        cf[MID, rows, :] = m
        cf[TOP, rows, :] = top
        cf[DIF, rows, :] = dif
        cf[KG, rows, :] = kg
        cf[GM, rows, :] = gm
        cf[W3, rows, :] = w3
        cf[C0, rows, :] = jnp.where(low_lanes, 0.0, c0)
        cf[F4, rows, :] = f4
        cf[GA2, rows, :] = ga2
        cf[U1, rows, :] = jnp.where(low_lanes, a * m2, b2)
        cf[U2, rows, :] = jnp.where(low_lanes, a * m, b1)
        cf[U3, rows, :] = jnp.where(low_lanes, a, b4)
        cf[U4, rows, :] = jnp.where(low_lanes, w3, b3)
        cf[B4, rows, :] = b4
        return carry

    lax.fori_loop(0, n // ROWS, coefficients, 0)

    mine = pl.ds(pl.multiple_of(core * half_n + z * zr, zr), zr)
    top_own, c0_own = cf[TOP, mine, :], cf[C0, mine, :]
    chip_gain, chip_mix = top_own * top_own, 2.0 * c0_own * top_own
    power, mix = jnp.ones_like(chip_gain), jnp.zeros_like(chip_gain)
    for k in range(nz + 1):
        hz[k] = power
        cz[k] = mix
        power, mix = power * chip_gain, mix * chip_gain + power * chip_mix
    told(1)
    tell(2)

    def correct(m, top, entry, r):
        p1 = m * entry + r[0]
        p2 = m * p1 + r[1]
        p3 = m * p2 + r[2]
        q = m * (m * (m * r[0] + r[1]) + r[2]) + r[3]
        return [p1, p2, p3, top * entry + q]

    def iterations(rows, b, b4p, bkp, e1, e2):
        a, m, top = cf[A4, rows, :], cf[MID, rows, :], cf[TOP, rows, :]
        dif, gm = cf[DIF, rows, :], cf[GM, rows, :]
        d4p = cf[KG, rows, :] * e1 + bkp
        r1 = [a * b4p, a * b[0], a * b[1], a * b[2]]
        k1 = correct(m, top, e1, r1)
        v1 = [b[c] + k1[c] for c in range(4)]
        d = [dif * e1, dif * k1[0], dif * k1[1], dif * k1[2] - gm * e1]
        r2 = [a * d4p, a * d[0], a * d[1], a * d[2]]
        k2 = correct(m, top, e2, r2)
        v2 = [v1[c] + d[c] + k2[c] for c in range(4)]
        v0 = b4p + e1 + d4p + e2
        return r1, k1, v1, r2, k2, v2, v0

    def paired(points, h):
        at = jnp.where(low_lanes, points[2 * h], swap(points[2 * h + 1]))
        end = jnp.where(low_lanes, points[2 * h + 1], swap(points[2 * h + 2]))
        return at, end

    def relax(h, start_row, parts):
        for i in range(parts):
            rows = pl.ds(pl.multiple_of(start_row + i * ROWS, ROWS), ROWS)
            g = cf[GAIN, rows, :]
            v = None
            for j in range(4):
                s = g * src[h, rows, 128 * j : 128 * j + 128]
                src[h, rows, 128 * j : 128 * j + 128] = s
                v = s if v is None else g * v + s
            if h == 0:
                v = v + cf[A4, rows, :] * u0[rows, :]
            w = swap(v)
            ab[h, rows, :] = v
            ab[2 + h, rows, :] = w
            t = cf[U1 + 2 * h, rows, :] * v + cf[U2 + 2 * h, rows, :] * w
            tt[rows, :] = t if h == 0 else tt[rows, :] + t

    own_row = pl.multiple_of(core * half_n, half_n)
    other_row = pl.multiple_of((1 - core) * half_n, half_n)
    own, other = pl.ds(own_row, half_n), pl.ds(other_row, half_n)
    u0[...] = jnp.zeros_like(u0)

    for k in range(1, ny):
        yf_from(0, k).wait_recv()
    src[0] = jnp.dot(table[0], rbuf[0].reshape(n, 512), preferred_element_type=f32)

    @pl.when(first)
    def _():
        for k in range(1, ny):
            y0_from(k).wait_recv()
        r0buf[y] = s0buf[y]
        u0[...] = jnp.dot(table[0], r0buf[...].reshape(n, 128), preferred_element_type=f32)

    relax(0, 0, n // ROWS)
    for k in range(1, ny):
        yf_from(1, k).wait_recv()
    src[1] = jnp.dot(table[0], rbuf[1].reshape(n, 512), preferred_element_type=f32)
    relax(1, other_row, half_n // ROWS)

    join = remote(tt.at[other], cbuf, dsend_s.at[0], drecv_s.at[0], partner)
    join.start()
    relax(1, own_row, half_n // ROWS)

    wide = lax.broadcasted_iota(jnp.int32, (half_n, 128), 1) < 64
    nsend[0] = jnp.where(wide, ab[3, 0:half_n, :], ab[1, half_n:n, :])

    def pass_on(k):
        return remote(nsend.at[k], nbuf.at[k], nsend_s.at[k], nrecv_s.at[k], place(after))

    @pl.when(jnp.logical_not(last))
    def _():
        pass_on(0).start()

    @pl.when(first)
    def _():
        nbuf[...] = jnp.zeros_like(nbuf)

    join.wait_recv()
    own_t, got_t = tt[own, :], cbuf[...]
    early = jnp.where(core == 0, own_t, got_t)
    late = jnp.where(core == 0, got_t, own_t)
    top_half, c0_half = cf[TOP, own, :], cf[C0, own, :]
    joined = top_half * early + c0_half * swap(early) + late
    tc[...] = joined.reshape(nz, zr, 128)

    def zs(k):
        to = lax.rem(z + k, nz)
        return remote(tc.at[to], zbuf.at[z], zsend_s.at[k], zrecv_s.at[k], {"tm_1": to})

    def zs_from(k):
        frm = lax.rem(z + nz - k, nz)
        return remote(tc.at[frm], zbuf.at[frm], zsend_s.at[k], zrecv_s.at[k], {"tm_1": frm})

    told(2)
    for k in zorder:
        zs(k).start()
    zbuf[z] = tc[z]

    @pl.when(jnp.logical_not(first))
    def _():
        pass_on(0).wait_recv()

    def unpack(k, i, rows):
        v = nbuf[k, pl.ds(pl.multiple_of(lax.rem(i, n // ROWS // 2) * ROWS, ROWS), ROWS), :]
        return jnp.where(i < n // ROWS // 2, v, swap(v))

    def follow(i, carry):
        rows = pl.ds(pl.multiple_of(i * ROWS, ROWS), ROWS)
        top_rows = pl.ds(pl.multiple_of(half_n + i * ROWS, ROWS), ROWS)
        v = nbuf[0, rows, :]

        def part(r, b4p):
            ga2 = cf[GA2, r, :]
            out = cf[F4, r, :] * b4p + cf[MID, r, :] * ga2 * ab[0, r, :] + ga2 * ab[2, r, :]
            return out - cf[KG, r, :] * cf[A4, r, :] * ab[1, r, :]

        nsend[1, rows, :] = jnp.where(low_lanes, part(rows, v), swap(part(top_rows, swap(v))))
        return carry

    lax.fori_loop(0, n // ROWS // 2, follow, 0)

    @pl.when(jnp.logical_not(last))
    def _():
        pass_on(1).start()

    def responses(i, carry):
        rows = pl.ds(pl.multiple_of(i * ROWS, ROWS), ROWS)
        g = cf[GAIN, rows, :]
        none, unit = jnp.zeros_like(g), jnp.ones_like(g)
        for ref, e1, e2 in ((xc, unit, none), (yc, none, unit)):
            _, _, _, _, _, v2, v0 = iterations(rows, [none] * 4, none, none, e1, e2)
            for h in range(2):
                at, end = paired([v0] + v2, h)
                for j in range(4):
                    at = g * at if j < 3 else end
                    ref[h, rows, 128 * j : 128 * j + 128] = at
        return carry

    lax.fori_loop(0, n // ROWS, responses, 0)

    for k in range(1, nz):
        zs_from(k).wait_recv()

    local, states = jnp.zeros_like(chip_gain), []
    for k in range(nz):
        states.append(local)
        local = chip_gain * local + zbuf[k]
    total = local
    mixed, mixes = jnp.zeros_like(chip_gain), []
    for k in range(nz):
        mixes.append(mixed)
        mixed = chip_gain * mixed + chip_mix * swap(states[k])
    xsend[...] = total + mixed
    for k in range(nz):
        esend[k] = states[k] + mixes[k]

    def xs(k):
        return remote(xsend, xbuf.at[x], xsend_s.at[k], xrecv_s.at[k], {"tm_0": lax.rem(x + k, nx)})

    def xs_from(k):
        frm = lax.rem(x + nx - k, nx)
        return remote(xsend, xbuf.at[frm], xsend_s.at[k], xrecv_s.at[k], {"tm_0": frm})

    for k in range(1, nx):
        xs(k).start()
    for k in range(1, nx):
        xs_from(k).wait_recv()
    entering = jnp.zeros_like(chip_gain)
    for k in range(nx - 1):
        stepped = hz[nz] * entering + cz[nz] * swap(entering) + xbuf[k]
        entering = jnp.where(k < x, stepped, entering)
    turned = swap(entering)
    for k in range(nz):
        esend[k] = esend[k] + hz[k] * entering + cz[k] * turned

    def es(k):
        to = lax.rem(z + k, nz)
        return remote(esend.at[to], ebuf.at[z], esend_s.at[k], erecv_s.at[k], {"tm_1": to})

    def es_from(k):
        frm = lax.rem(z + nz - k, nz)
        return remote(esend.at[frm], ebuf.at[frm], esend_s.at[k], erecv_s.at[k], {"tm_1": frm})

    for k in zorder:
        es(k).start()
    ebuf[z] = esend[z]

    @pl.when(jnp.logical_not(first))
    def _():
        pass_on(1).wait_recv()

    def neighbours(i, rows):
        b4p, bkp = unpack(0, i, rows), unpack(1, i, rows)
        b = [ab[0, rows, :], ab[2, rows, :], ab[1, rows, :], ab[3, rows, :]]
        return b, b4p, bkp, cf[W3, rows, :] * b4p, cf[W3, rows, :] * bkp + cf[B4, rows, :] * b4p

    def still(i, carry):
        rows = pl.ds(pl.multiple_of(i * ROWS, ROWS), ROWS)
        b, b4p, bkp, c1, c2 = neighbours(i, rows)
        _, _, _, _, _, v2, v0 = iterations(rows, b, b4p, bkp, -c1, -c2)
        points = [jnp.where(first, u0[rows, :], v0)] + v2
        g = cf[GAIN, rows, :]
        for h in range(2):
            at, end = paired(points, h)
            for j in range(4):
                lanes = slice(128 * j, 128 * j + 128)
                at = g * at + src[h, rows, lanes] if j < 3 else end
                src[h, rows, lanes] = at
        return carry

    lax.fori_loop(0, n // ROWS, still, 0)

    for k in range(1, nz):
        es_from(k).wait_recv()

    chip = ebuf[...].reshape(half_n, 128)
    second = cf[TOP, own, :] * chip + cf[C0, own, :] * swap(chip) + jnp.where(core == 0, tt[own, :], cbuf[...])
    fsend[...] = jnp.where(core == 0, second, chip)
    est[own, :] = jnp.where(core == 0, chip, second)
    give = remote(fsend, fbuf, dsend_s.at[1], drecv_s.at[1], partner)
    give.start()
    give.wait_recv()
    est[other, :] = fbuf[...]

    def path(q):
        h, first_step = q // 2, 2 * (q % 2)
        for i in range(n // ROWS):
            rows = slice(i * ROWS, i * ROWS + ROWS)
            v = est[rows, :]
            w = swap(v)
            sx, sy = jnp.where(low_lanes, v, w), jnp.where(low_lanes, w, v)
            for j in range(first_step, first_step + 2):
                lanes = slice(128 * j, 128 * j + 128)
                at = src[h, rows, lanes] + xc[h, rows, lanes] * sx + yc[h, rows, lanes] * sy
                high = at.astype(bf16)
                phi[h, rows, lanes] = high
                plo[h, rows, lanes] = (at - high.astype(f32)).astype(bf16)


    def norms(i, carry):
        rows = pl.ds(pl.multiple_of(i * ROWS, ROWS), ROWS)
        b, b4p, bkp, c1, c2 = neighbours(i, rows)
        v = est[rows, :]
        r1, k1, v1, r2, k2, v2, _ = iterations(rows, b, b4p, bkp, v - c1, swap(v) - c2)
        for group, fields in enumerate((r1, r2, k1, k2, v1, v2)):
            for c in range(4):
                at = 4 * group + c
                sq = fields[c] * fields[c]
                stat[at : at + 1, :] = stat[at : at + 1, :] + jnp.sum(sq, axis=0, keepdims=True)
        return carry

    def ts(k):
        return remote(stat, stbuf.at[y], tsend_s.at[k], trecv_s.at[k], ypeer(k))

    def ts_from(k):
        frm = lax.rem(y + ny - k, ny)
        return remote(stat, stbuf.at[frm], tsend_s.at[k], trecv_s.at[k], ypeer(k))

    def og(h, k):
        to = lax.rem(y + k, ny)
        return remote(obuf.at[h, to], gbuf.at[h, y], osend_s.at[h, k], orecv_s.at[h, k], ypeer(k))

    def og_from(h, k):
        frm = lax.rem(y + ny - k, ny)
        return remote(obuf.at[h, frm], gbuf.at[h, frm], osend_s.at[h, k], orecv_s.at[h, k], ypeer(k))

    for q in range(4):
        path(q)
        h, lanes = q // 2, slice(256 * (q % 2), 256 * (q % 2) + 256)
        out = jnp.dot(table[0], phi[h, :, lanes], preferred_element_type=f32)
        out = out + jnp.dot(table[0], plo[h, :, lanes], preferred_element_type=f32)
        out = out + jnp.dot(table[1], phi[h, :, lanes], preferred_element_type=f32)
        obuf[q] = out.astype(bf16).reshape(ny, slab, 256)
        for k in yorder:
            og(q, k).start()
        if q == 1:
            stat[...] = jnp.zeros_like(stat)
            lax.fori_loop(0, n // ROWS, norms, 0)
            for k in yorder:
                ts(k).start()
    for q in range(4):
        gbuf[q, y] = obuf[q, y]
    stbuf[y] = stat[...]

    for q in range(4):
        for k in range(1, ny):
            og_from(q, k).wait_recv()
        lhs = jnp.concatenate(
            [
                jnp.concatenate([gbuf[q, s, :, 128 * j : 128 * j + 128] for s in range(ny)], axis=1)
                for j in range(2)
            ],
            axis=0,
        )
        for p in range(2):
            out = jnp.dot(lhs, pair_out[p], preferred_element_type=f32)
            for j in range(2):
                heat[8 * (q // 2) + 4 * p + 2 * (q % 2) + j] = out[j * slab : (j + 1) * slab, :]

    for k in range(1, ny):
        ts_from(k).wait_recv()
    sums = stbuf[0]
    for s in range(1, ny):
        sums = sums + stbuf[s]
    keep = lax.broadcasted_iota(jnp.int32, sums.shape, 1) < 64
    sums = jnp.sum(jnp.where(keep, sums, 0.0), axis=1, keepdims=True)
    residual = jnp.broadcast_to(jnp.sqrt(sums[0:8] / (n * n)), (8, 128))
    moved = jnp.broadcast_to(jnp.sqrt(sums[8:16] / sums[16:24]), (8, 128))
    spot = lax.broadcasted_iota(jnp.int32, (8, 128), 1) == lax.rem(lax.broadcasted_iota(jnp.int32, (8, 128), 0), 4)
    for ref, v in ((history, residual), (change, moved)):
        v = jnp.where(spot, v, 0.0)
        for it in range(2):
            ref[it : it + 1, :] = jnp.sum(v[4 * it : 4 * it + 4], axis=0, keepdims=True)[:, 0:4]

    for k in range(1, ny):
        for h in range(2):
            yf(h, k).wait_send()
        for q in range(4):
            og(q, k).wait_send()
        ts(k).wait_send()

    @pl.when(first)
    def _():
        for k in range(1, ny):
            y0(k).wait_send()

    join.wait_send()
    give.wait_send()

    @pl.when(jnp.logical_not(last))
    def _():
        pass_on(0).wait_send()
        pass_on(1).wait_send()

    for k in range(1, nz):
        zs(k).wait_send()
        es(k).wait_send()
    for k in range(1, nx):
        xs(k).wait_send()

def store(heat_v, history_v, change_v, heat, history, change, sems):
    cut = [pl.ds(4 * i, 4) for i in range(STEPS // 4)]
    pairs = [(heat_v.at[c], heat.at[c]) for c in cut] + [(history_v, history), (change_v, change)]
    copies = [pltpu.make_async_copy(a, b, sems.at[i]) for i, (a, b) in enumerate(pairs)]
    for copy in copies:
        copy.start()
    for copy in copies:
        copy.wait()

def per_device(dims, forcing, starting_heat):
    nx, nz, nc, ny, n = dims
    slab, half_n, zr = n // ny, n // 2, n // 2 // nz
    bf16, f32 = jnp.bfloat16, jnp.float32
    consts = tables(n, ny)
    dma = pltpu.SemaphoreType.DMA
    scratch = [
        ((STEPS, slab, n), bf16),
        ((slab, n), bf16),
    ]
    scratch += [(c.shape, c.dtype) for c in consts]
    scratch += [
        ((2, ny, slab, 512), bf16),
        ((2, ny, slab, 512), bf16),
        ((ny, slab, 128), bf16),
        ((ny, slab, 128), bf16),
        ((2, n, 512), f32),
        ((2, n, 512), f32),
        ((2, n, 512), f32),
        ((n, 128), f32),
        ((16, n, 128), f32),
        ((4, n, 128), f32),
        ((n, 128), f32),
        ((half_n, 128), f32),
        ((nz, zr, 128), f32),
        ((nz, zr, 128), f32),
        ((nz + 1, zr, 128), f32),
        ((nz + 1, zr, 128), f32),
        ((zr, 128), f32),
        ((nx, zr, 128), f32),
        ((nz, zr, 128), f32),
        ((nz, zr, 128), f32),
        ((half_n, 128), f32),
        ((half_n, 128), f32),
        ((2, half_n, 128), f32),
        ((2, half_n, 128), f32),
        ((n, 128), f32),
        ((2, n, 512), bf16),
        ((2, n, 512), bf16),
        ((4, ny, slab, 256), bf16),
        ((4, ny, slab, 256), bf16),
        ((24, 128), f32),
        ((ny, 24, 128), f32),
    ]
    sems = [
        (2, ny), (2, ny), (ny,), (ny,), (2,), (2,), (2,), (2,), (nz,), (nz,),
        (nx,), (nx,), (nz,), (nz,), (4, ny), (4, ny), (ny,), (ny,), (7,),
    ]
    vmem = pl.BlockSpec(memory_space=pltpu.VMEM)
    hbm = pl.BlockSpec(memory_space=pltpu.HBM)
    shapes = ((STEPS, slab, n), (2, 4), (2, 4))
    held = pl.pallas_call(
        functools.partial(kernel, dims),
        out_shape=tuple(pltpu.VMEM(s, f32) for s in shapes),
        in_specs=[hbm] * 7,
        out_specs=(vmem, vmem, vmem),
        scratch_shapes=[pltpu.VMEM(s, d) for s, d in scratch]
        + [dma(s) for s in sems]
        + [pltpu.SemaphoreType.REGULAR((4,))],
        compiler_params=pltpu.CompilerParams(
            collective_id=0, has_side_effects=True, vmem_limit_bytes=VMEM_GRANT
        ),
    )(forcing, starting_heat, *[jnp.asarray(c) for c in consts])
    return pl.pallas_call(
        store,
        out_shape=tuple(jax.ShapeDtypeStruct(s, f32) for s in shapes),
        in_specs=[vmem] * 3,
        out_specs=(hbm, hbm, hbm),
        scratch_shapes=[dma((STEPS // 4 + 2,))],
        compiler_params=pltpu.CompilerParams(vmem_limit_bytes=4 * 1024 * 1024),
    )(*held)

def build(mesh, nx, nz, nc, n):
    ny = mesh.shape["space"]
    torus = Mesh(mesh.devices.reshape(nx, nz, nc, ny), TM + ("space",))
    return jax.shard_map(
        functools.partial(per_device, (nx, nz, nc, ny, n)),
        mesh=torus,
        in_specs=(P(TM, "space", None), P("space", None)),
        out_specs=(P(TM, "space", None), P(None, TM), P(None, TM)),
        check_vma=False,
    )

def solution(mesh):
    return build(mesh, 4, 16, 2, 256)
```
